32 devices in a mesh: client: 32 (over z, y, x, core).
Axes of the slice: x: 2, y: 2, z: 4, core: 2. Of those that a mesh axis runs over, the one named last changes fastest.
Arguments:
- patches: bfloat16 [4096, 192], P('client'), may hold values from -6 to 6
- labels: int32 [256], replicated, may hold values from 0 to 9
- assign: int32 [32, 1], replicated, may hold values from 0 to 15; in each aligned block of 32 rows (0 to 31, 32 to 63, ...) at most 4 rows name the same one
- patch_embed: bfloat16 [192, 384], replicated, may hold values from -0.4375 to 0.4375
- positions: bfloat16 [16, 384], replicated, may hold values from -3 to 3
- client_in: bfloat16 [384, 3072], replicated, may hold values from -3 to 3
- client_down: bfloat16 [1536, 384], replicated, may hold values from -0.15625 to 0.15625
- server_in: bfloat16 [2, 6144, 3072], P(None, 'client'), may hold values from -3 to 3
- server_down: bfloat16 [2, 24576, 384], P(None, 'client'), may hold values from -0.15625 to 0.15625
- classifier: bfloat16 [16, 384, 10], replicated, may hold values from -15 to 15
Outputs:
- losses: float32 [32, 16], P('client')
- grad_patch_embed: float32 [192, 384], P(None, 'client')
- grad_positions: float32 [16, 384], P(None, 'client')
- grad_client_in: float32 [384, 3072], P(None, 'client')
- grad_client_down: float32 [1536, 384], P(None, 'client')
- grad_server_in: float32 [2, 6144, 3072], P(None, 'client')
- grad_server_down: float32 [2, 24576, 384], P(None, 'client')
- grad_classifier: float32 [6144, 10], P('client')
The draws below stay inside these ranges and needn't reach their ends.
Inputs may be any that keep to these rules, and one draw needn't show every extreme that they name: `assign`: no server shard is named by more than 4 clients, a bound that some block reaches.
All inputs are finite; a program needn't handle non-finite values.
Results may differ from the reference program's by a relative error of at most 0.025.
Values may be sent and summed in bfloat16 or wider, within the bound.
No kernel may reach another device: no remote copies, remote signals or barrier semaphores. Data moves between devices by JAX's collectives and lax.ppermute only.
A program may use at most 128 MiB of HBM per device.

```python
import math
import jax
import jax.numpy as jnp
import numpy as np
from jax import lax

D = 384
HEADS = 6
FF = 1536
PATCH = 192
TOK = 16
CLASSES = 10
IMG = 8
SHARDS = 16
SLOTS = 2
SERVER_LAYERS = 2
CAPACITY = 4
N_CLIENT = 32


def scaled_normal(key, shape, fan_in):
    return jax.random.truncated_normal(key, -4.0, 4.0, shape, jnp.float32) / math.sqrt(fan_in)


def draw_client_in(key, part):
    values = scaled_normal(jax.random.fold_in(key, 11), (D, 4 * D + FF), D)
    return values.astype(jnp.bfloat16)


def draw_server_in(key, part):
    values = scaled_normal(jax.random.fold_in(key, 23), (SERVER_LAYERS, SHARDS * D, 4 * D + FF), D)
    return values.astype(jnp.bfloat16)


def draw_classifier(key, part):
    values = scaled_normal(jax.random.fold_in(key, 37), (SHARDS, D, CLASSES), D)
    return values.astype(jnp.bfloat16)


def place_ends(result, key, least, high):
    dims = result.shape
    place = [jax.random.randint(jax.random.fold_in(key, axis), (), 0, dims[axis]) for axis in range(len(dims))]
    result = result.at[tuple(place)].set(least)
    longest = dims.index(max(dims))
    place[longest] = (place[longest] + 1) % dims[longest]
    return result.at[tuple(place)].set(high)


def levels(key, extent, split, least, top_value):
    level, own = 1.0, jax.random.fold_in(key, 6)
    for dim, blocks in split:
        steps = jnp.exp(jax.random.uniform(jax.random.fold_in(own, dim), (blocks,), jnp.float32, least / len(split), top_value / len(split)))
        level = level * jnp.repeat(steps, extent[dim] // blocks).reshape([-1 if axis == dim else 1 for axis in range(len(extent))])
    return level


def assign_block(stream_key, own, number, rows, amount, top, reach, lean):
    sequence = jax.random.permutation(stream_key, amount)
    heavy_load, common = shares(amount, rows * top, reach, lean, True), shares(amount, rows * top, reach, lean, False)
    places = jnp.arange(amount)

    def named(sizes, rotation):
        used = int((sizes > 0).sum())
        fixed = max(1, used // 4)
        shifted = fixed + (places - fixed + rotation * (used - fixed)) % max(1, amount - fixed)
        return jnp.zeros((amount,), jnp.int32).at[sequence[jnp.where(places < fixed, places, shifted)]].set(jnp.asarray(sizes, jnp.int32))

    sizes = jnp.where(number % 4 == 0, named(heavy_load, number // 4), named(common, number - number // 4 - 1))
    mixed = jax.random.permutation(jax.random.fold_in(own, 3), amount)
    donor, sink = mixed[0:amount // 2 * 2:2], mixed[1:amount // 2 * 2:2]
    margin = jnp.minimum(sizes[donor] - 1, reach - sizes[sink]) // 2
    margin = jnp.where((donor == sequence[0]) | (sink == sequence[0]) | (sizes[sink] == 0), 0, jnp.maximum(margin, 0))
    shifted = jax.random.randint(jax.random.fold_in(own, 4), (amount // 2,), 0, 1 << 20) % (margin + 1)
    sizes = sizes.at[donor].add(-shifted).at[sink].add(shifted)
    items = jnp.searchsorted(jnp.cumsum(sizes), jnp.arange(rows * top), side="right").astype(jnp.int32)
    grid = items.reshape(top, rows).T
    grid = grid[jax.random.permutation(jax.random.fold_in(own, 1), rows)]
    rotation = jax.random.randint(jax.random.fold_in(own, 2), (rows, 1), 0, top)
    return jnp.take_along_axis(grid, (jnp.arange(top)[None, :] + rotation) % top, axis=1)


def shares(count, total, reach, slope, full):
    weights = [(1 << 20) // math.isqrt(rank ** slope) + 1 for rank in range(1, count + 1)]
    largest = reach if full else min(reach, max(-(-total // count), total * weights[0] // sum(weights)))
    least = 1 if total - largest >= count - 1 else 0
    given, spare = [largest] + [least] * (count - 1), total - largest - least * (count - 1)
    while spare > 0:
        candidates = [i for i in range(1, count) if given[i] < largest] or [i for i in range(1, count) if given[i] < reach]
        mass, remaining = sum([weights[i] for i in candidates]), spare
        for i in candidates:
            addition = min(reach - given[i], max(1, remaining * weights[i] // mass), spare)
            given[i] = given[i] + addition
            spare = spare - addition
    return np.array(given)


def normal_values(rng, extent, scale, bound, cuts=(), kind=jnp.bfloat16):
    entries = jax.random.normal(rng, extent, jnp.float32) * scale
    if len(cuts) > 0:
        entries = levels(rng, extent, cuts, -0.22, 0.18) * entries
    return jnp.clip(entries, min=-bound, max=bound).astype(kind)


def setup_inputs(seed: int = 0) -> dict:
    splits = jax.random.split(jax.random.key(seed), 11)
    patches = normal_values(splits[0], (N_CLIENT * IMG * TOK, PATCH), 1.0, 6.0, ((0, 32),))
    labels = place_ends(jax.random.randint(splits[1], (N_CLIENT * IMG,), 0, CLASSES), jax.random.fold_in(splits[1], 1), 0, CLASSES - 1).astype(jnp.int32)
    assign_keys = jax.random.split(jax.random.fold_in(splits[2], 1), N_CLIENT // N_CLIENT)
    assign_turns = jax.random.permutation(jax.random.fold_in(splits[2], 3), N_CLIENT // N_CLIENT)
    assign = jax.vmap(lambda own, number: assign_block(jax.random.fold_in(splits[2], 2), own, number, N_CLIENT, SHARDS, 1, CAPACITY, 2))(assign_keys, assign_turns).reshape((N_CLIENT, 1))
    patch_embed = normal_values(splits[3], (PATCH, D), PATCH ** -0.5, 0.4375)
    positions = normal_values(splits[4], (TOK, D), 0.5, 3.0)
    client_in = draw_client_in(jax.random.fold_in(splits[10], 71), 0)
    client_down = normal_values(splits[6], (FF, D), FF ** -0.5, 0.15625)
    server_in = draw_server_in(jax.random.fold_in(splits[10], 71), 0)
    server_down = normal_values(splits[8], (SERVER_LAYERS, SHARDS * FF, D), FF ** -0.5, 0.15625, ((1, 32),))
    classifier = draw_classifier(jax.random.fold_in(splits[10], 71), 0)
    return dict(patches=patches, labels=labels, assign=assign, patch_embed=patch_embed, positions=positions, client_in=client_in, client_down=client_down, server_in=server_in, server_down=server_down, classifier=classifier)


EPSILON = 1e-06

def layer_norm(inputs):
    centre = inputs - lax.optimization_barrier(jnp.mean(inputs, axis=-1, keepdims=True))
    spread = lax.optimization_barrier(jnp.mean(centre * centre, axis=-1, keepdims=True))
    return centre * lax.rsqrt(spread + EPSILON)

def encoder_block(stream, weight_in, weight_down):
    images, tokens, model_width = stream.shape
    head_dim = model_width // HEADS
    normed = layer_norm(stream).astype(jnp.bfloat16).reshape(images * tokens, model_width)
    projected = jnp.dot(normed, weight_in[:, :3 * model_width], preferred_element_type=jnp.float32)
    projected = projected.reshape(images, tokens, 3, HEADS, head_dim)
    queries = projected[:, :, 0]
    key_rows = projected[:, :, 1]
    values = projected[:, :, 2]
    scores = jnp.einsum('bqhe,bkhe->bhqk', queries, key_rows, precision=lax.Precision.HIGHEST) / math.sqrt(head_dim)
    weights_attn = jax.nn.softmax(scores, axis=-1)
    attended = jnp.einsum('bhqk,bkhe->bqhe', weights_attn, values, precision=lax.Precision.HIGHEST)
    attended = attended.reshape(images * tokens, model_width).astype(jnp.bfloat16)
    stream = stream + jnp.dot(attended, weight_in[:, 3 * model_width:4 * model_width], preferred_element_type=jnp.float32).reshape(images, tokens, model_width)
    normed = layer_norm(stream).astype(jnp.bfloat16).reshape(images * tokens, model_width)
    hidden = jax.nn.gelu(jnp.dot(normed, weight_in[:, 4 * model_width:], preferred_element_type=jnp.float32)).astype(jnp.bfloat16)
    return stream + jnp.dot(hidden, weight_down, preferred_element_type=jnp.float32).reshape(images, tokens, model_width)

def client_forward(patch_rows, patch_embed, positions, client_in, client_down):
    stream = jnp.dot(patch_rows, patch_embed, preferred_element_type=jnp.float32).reshape(-1, TOK, D)
    stream = stream + positions.astype(jnp.float32)
    stream = encoder_block(stream, client_in, client_down)
    return stream.reshape(-1, D).astype(jnp.bfloat16)

def server_loss(cut_rows, slot_hot, weights_in, weights_down, class_shard):
    stream = cut_rows.astype(jnp.float32).reshape(-1, TOK, D)
    for layer in range(len(weights_in)):
        stream = encoder_block(stream, weights_in[layer], weights_down[layer])
    pooled = layer_norm(lax.optimization_barrier(jnp.mean(stream, axis=1))).astype(jnp.bfloat16)
    logits = jnp.dot(pooled, class_shard, preferred_element_type=jnp.float32)
    per_loss = (jax.nn.logsumexp(logits, axis=-1) - lax.optimization_barrier(jnp.sum(slot_hot * logits, axis=-1))) * lax.optimization_barrier(jnp.sum(slot_hot, axis=-1))
    return (jnp.sum(per_loss), per_loss)

def arrival_rank(routes):
    places = jnp.arange(routes.shape[0], dtype=jnp.int32)
    earlier = (routes[:, None] == routes[None, :]) & (places[:, None] < places[None, :])
    return lax.optimization_barrier(jnp.sum(earlier.astype(jnp.int32), axis=0))

def select_matrix(routes, arrival, shard, capacity):
    slots_here = jnp.arange(capacity, dtype=jnp.int32)[:, None]
    return ((routes[None, :] == shard) & (arrival[None, :] == slots_here)).astype(jnp.bfloat16)

def slot_labels(labels, selector, rank_in_group, per_image, members):
    label_table = labels.reshape(members, IMG)
    label_part = lax.dynamic_slice_in_dim(label_table, (rank_in_group * per_image).astype(jnp.int32), per_image, 1)
    onehot = (label_part[:, :, None] == jnp.arange(CLASSES, dtype=jnp.int32)[None, None, :]).astype(jnp.float32)
    onehot = onehot.reshape(members, per_image * CLASSES)
    chosen = jnp.dot(selector.astype(jnp.float32), onehot, precision=lax.Precision.HIGHEST)
    return chosen.reshape(-1, CLASSES)

def reference(patches, labels, assign, patch_embed, positions, client_in, client_down, server_in, server_down, classifier):
    members = N_CLIENT
    group_size = members // SHARDS
    per_image = IMG // group_size
    piece_rows = IMG * TOK // group_size
    capacity = SLOTS * group_size
    width_all = 4 * D + FF
    routes = assign[:, 0]
    arrival = arrival_rank(routes)
    patch_sets = patches.reshape(members, IMG * TOK, PATCH)

    def client_cut(patch_rows):
        return client_forward(patch_rows, patch_embed, positions, client_in, client_down)
    cuts = lax.map(client_cut, patch_sets)
    cut_pieces = cuts.reshape(members, group_size, piece_rows * D)
    shard_in = server_in.reshape(SERVER_LAYERS, SHARDS, D, width_all)
    shard_down = server_down.reshape(SERVER_LAYERS, SHARDS, FF, D)

    def device_step(carry, device):
        acc_in, acc_down, acc_class = carry
        shard = device // group_size
        rank_in_group = device % group_size
        selector = select_matrix(routes, arrival, shard, capacity)
        own_piece = lax.dynamic_index_in_dim(cut_pieces, rank_in_group, 1, keepdims=False)
        compact = jnp.dot(selector, own_piece, preferred_element_type=jnp.float32).astype(jnp.bfloat16)
        compact = compact.reshape(capacity * piece_rows, D)
        slot_hot = slot_labels(labels, selector, rank_in_group, per_image, members)
        layer_in = lax.dynamic_index_in_dim(shard_in, shard, 1, keepdims=False)
        layer_down = lax.dynamic_index_in_dim(shard_down, shard, 1, keepdims=False)
        class_shard = lax.dynamic_index_in_dim(classifier, shard, 0, keepdims=False)

        def loss_of(cut_rows, weights_in, weights_down, class_weights):
            return server_loss(cut_rows, slot_hot, weights_in, weights_down, class_weights)
        list_in = tuple((layer_in[layer] for layer in range(SERVER_LAYERS)))
        list_down = tuple((layer_down[layer] for layer in range(SERVER_LAYERS)))
        total_loss, server_back, per_loss = jax.vjp(loss_of, compact, list_in, list_down, class_shard, has_aux=True)
        grad_cut, grad_in, grad_down, grad_class = server_back(jnp.ones((), jnp.float32))
        acc_in = acc_in.at[:, shard].add(jnp.stack(grad_in).astype(jnp.float32))
        acc_down = acc_down.at[:, shard].add(jnp.stack(grad_down).astype(jnp.float32))
        acc_class = acc_class.at[shard].add(grad_class.astype(jnp.float32))
        return ((acc_in, acc_down, acc_class), (grad_cut, per_loss))
    start = (jnp.zeros((SERVER_LAYERS, SHARDS, D, width_all), jnp.float32), jnp.zeros((SERVER_LAYERS, SHARDS, FF, D), jnp.float32), jnp.zeros((SHARDS, D, CLASSES), jnp.float32))
    sums, outputs = lax.scan(device_step, start, jnp.arange(members, dtype=jnp.int32))
    acc_in, acc_down, acc_class = sums
    cut_grads, loss_rows = outputs
    cut_grads = cut_grads.reshape(SHARDS, group_size, capacity, piece_rows * D)

    def client_step(carry, client):
        shard = routes[client]
        slot = arrival[client]
        by_shard = lax.dynamic_index_in_dim(cut_grads, shard, 0, keepdims=False)
        own_grads = lax.dynamic_index_in_dim(by_shard, slot, 1, keepdims=False).reshape(IMG * TOK, D)
        patch_rows = lax.dynamic_index_in_dim(patch_sets, client, 0, keepdims=False)

        def client_of(embed_weights, position_weights, in_weights, down_weights):
            return client_forward(patch_rows, embed_weights, position_weights, in_weights, down_weights)
        cut_again, client_back = jax.vjp(client_of, patch_embed, positions, client_in, client_down)
        grads = client_back(own_grads)
        return (tuple((total + part_grad.astype(jnp.float32) for total, part_grad in zip(carry, grads))), None)
    client_start = (jnp.zeros((PATCH, D), jnp.float32), jnp.zeros((TOK, D), jnp.float32), jnp.zeros((D, width_all), jnp.float32), jnp.zeros((FF, D), jnp.float32))
    client_sums, unused = lax.scan(client_step, client_start, jnp.arange(members, dtype=jnp.int32))
    return (loss_rows, client_sums[0], client_sums[1], client_sums[2], client_sums[3], acc_in.reshape(SERVER_LAYERS, SHARDS * D, width_all), acc_down.reshape(SERVER_LAYERS, SHARDS * FF, D), acc_class.reshape(SHARDS * D, CLASSES))
```

```python
import math

import jax
import jax.numpy as jnp
from jax import lax
from jax.experimental import pallas as pl
from jax.experimental.pallas import tpu as pltpu
from jax.sharding import PartitionSpec as P

HEADS = 6
SHARDS = 16
SLOTS = 2
EPSILON = 1e-06
BF = jnp.bfloat16
F32 = jnp.float32
GELU_A = math.sqrt(2.0 / math.pi)
GELU_B = 0.044715
LANES = 128
ROWS16 = 16


def mm(a, b):
    return lax.dot_general(a, b, (((1,), (0,)), ((), ())), preferred_element_type=F32)


def mm_nt(a, b):
    return lax.dot_general(a, b, (((1,), (1,)), ((), ())), preferred_element_type=F32)


def mm_tn(a, b):
    return lax.dot_general(a, b, (((0,), (0,)), ((), ())), preferred_element_type=F32)


def norm_forward(x):
    centre = x - jnp.mean(x, axis=-1, keepdims=True)
    spread = jnp.mean(centre * centre, axis=-1, keepdims=True)
    scale = lax.rsqrt(spread + EPSILON)
    return centre * scale, scale


def norm_backward(grad, normed, scale):
    mean_grad = jnp.mean(grad, axis=-1, keepdims=True)
    mean_both = jnp.mean(grad * normed, axis=-1, keepdims=True)
    return scale * (grad - mean_grad - normed * mean_both)


def stage_orders(bits):
    even = list(range(1, bits))
    odd = [3, 1, 4, 2] if bits == 5 else even[len(even) // 2 :] + even[: len(even) // 2]
    return even, odd


def slot_of_chip(offset, core, bits):
    even, odd = stage_orders(bits)
    total = bits - 1

    def place(order):
        value = 0
        for step, bit in enumerate(order):
            value = value | (((offset >> (bit - 1)) & 1) << (total - 1 - step))
        return value

    return jnp.where(core == 0, place(even), place(odd))


def split_rows(x, mask):
    return jnp.concatenate([jnp.where(mask, x, 0.0), jnp.where(mask, 0.0, x)], axis=0)


def make_chain(cfg):
    d, ff, tok = cfg["d"], cfg["ff"], cfg["tok"]
    members, group, capacity, pr = cfg["members"], cfg["group"], cfg["capacity"], cfg["pr"]
    images, classes, patch = cfg["images"], cfg["classes"], cfg["patch"]
    layers, bits = cfg["layers"], cfg["bits"]
    rows = capacity * pr
    per_image = pr // tok
    rows_in, rows_down = d // group, ff // group
    cin, cin_pad = cfg["cin"], cfg["cin_pad"]
    chips = members // 2
    halves = rows // LANES
    pairs = d // LANES
    pieces = cfg["pieces"]
    dpc = d // members
    chunk = d
    packed = cfg["packed"]

    def kernel(*refs):
        (assign, labels, arrived, embed, positions, client_in, client_down), refs = refs[:7], refs[7:]
        piece_in, refs = refs[: len(pieces)], refs[len(pieces) :]
        piece_down, refs = refs[: len(pieces)], refs[len(pieces) :]
        classifier, refs = refs[0], refs[1:]
        (losses, dcls, keep_out, send_out), refs = refs[:4], refs[4:]
        saved_out, refs = refs[:8], refs[8:]
        (w_in, w_down, pat, slot, x_ref, y_ref, qkv_f, qkv_b, prob, gp, r1, r2), refs = (
            refs[:12],
            refs[12:],
        )
        saved_refs = refs[:8]
        (c_u, c_o, c_u2, c_h, c_dqkv, c_dy, c_dpre, c_dout, pcat, dob_pad, keep, send), refs = (
            refs[:12],
            refs[12:],
        )
        (sems,) = refs

        me = lax.axis_index("client")
        rank = me % group
        shard = me // group
        core = me % 2

        def weight_copies(layer):
            if layer == 0:
                return [
                    pltpu.make_async_copy(client_in, w_in.at[0], sems.at[0]),
                    pltpu.make_async_copy(client_down, w_down.at[0], sems.at[1]),
                ]
            out = []
            base = 2 + (layer - 1) * 2 * group
            for number, (src_in, src_down, first, count) in enumerate(
                zip(piece_in, piece_down, cfg["first"], pieces)
            ):
                for inner in range(count):
                    index = first + inner
                    owner = rank ^ index
                    at_in = pl.multiple_of(owner * rows_in, rows_in)
                    at_down = pl.multiple_of(owner * rows_down, rows_down)
                    out.append(
                        pltpu.make_async_copy(
                            src_in.at[inner, layer - 1],
                            w_in.at[layer, pl.ds(at_in, rows_in)],
                            sems.at[base + 2 * index],
                        )
                    )
                    out.append(
                        pltpu.make_async_copy(
                            src_down.at[inner, layer - 1],
                            w_down.at[layer, pl.ds(at_down, rows_down)],
                            sems.at[base + 2 * index + 1],
                        )
                    )
            return out

        first_other = 2 + (layers - 1) * 2 * group

        def saved_copies(layer):
            base = first_other + capacity + (layer - 1) * 8
            return [
                pltpu.make_async_copy(src.at[layer], dst.at[layer - 1], sems.at[base + i])
                for i, (src, dst) in enumerate(zip(saved_refs, saved_out))
            ]

        def grad_copies(number, first, count):
            base = first_other + capacity + (layers - 1) * 8 + 2 * number
            at = pl.ds(first, count)
            return [
                pltpu.make_async_copy(keep.at[:, at], keep_out.at[:, at], sems.at[base]),
                pltpu.make_async_copy(send.at[:, at], send_out.at[:, at], sems.at[base + 1]),
            ]

        for k in range(capacity):
            slot[k] = 0

        def scan(c, count):
            hit = (assign[c] == shard) & (count < capacity)

            @pl.when(hit)
            def _():
                slot[count] = c

            return count + hit.astype(jnp.int32)

        filled = lax.fori_loop(0, members, scan, jnp.int32(0))
        pat_copies = [
            pltpu.make_async_copy(arrived.at[slot[k]], pat.at[k], sems.at[first_other + k])
            for k in range(capacity)
        ]
        for copy in pat_copies:
            copy.start()
        for layer in range(layers):
            for copy in weight_copies(layer):
                copy.start()
        for copy in pat_copies:
            copy.wait()

        half_mask = lax.broadcasted_iota(jnp.int32, (LANES, LANES), 1) < LANES // 2
        width_slot = LANES // group
        lane = lax.broadcasted_iota(jnp.int32, (packed, LANES), 1)
        for v in range(halves):
            blocks = [pat[v * group + t].astype(F32) for t in range(group)]
            for part in range(group):
                value = blocks[0]
                for t in range(group):
                    moved = pltpu.roll(blocks[t], (width_slot * (t - part)) % LANES, 1)
                    value = jnp.where(lane // width_slot == t, moved, value)
                pcat[part * packed : (part + 1) * packed, v * LANES : (v + 1) * LANES] = value.astype(BF)
        token = lax.broadcasted_iota(jnp.int32, (tok, rows), 1) % tok
        pcat[patch:] = (token == lax.broadcasted_iota(jnp.int32, (tok, rows), 0)).astype(F32).astype(BF)
        x_ref[...] = mm_tn(pcat[...], jnp.concatenate([embed[...], positions[...]], axis=0))

        row_slot = lax.broadcasted_iota(jnp.int32, (rows, 1), 0) // pr
        col_block = lax.broadcasted_iota(jnp.int32, (2 * LANES, LANES), 1) // tok
        row_block = (lax.broadcasted_iota(jnp.int32, (2 * LANES, LANES), 0) % LANES) // tok
        block_mask = col_block == row_block

        def forward(layer, carry):
            for which in range(layers):

                @pl.when(layer == which)
                def _(which=which):
                    for copy in weight_copies(which):
                        copy.wait()

            x = x_ref[...]
            normed, scale = norm_forward(x)
            u = normed.astype(BF)
            c_u[layer] = u
            r1[layer] = scale
            for part in range(3):
                value = mm(u, w_in[layer, :, part * d : (part + 1) * d])
                qkv_f[:, part * d : (part + 1) * d] = value
                qkv_b[layer, :, part * d : (part + 1) * d] = value.astype(BF)
            head_dim = d // HEADS
            for g in range(halves):
                rs = slice(g * LANES, (g + 1) * LANES)
                for p in range(pairs):
                    q = qkv_f[rs, p * LANES : (p + 1) * LANES] * (1.0 / math.sqrt(head_dim))
                    k = qkv_f[rs, d + p * LANES : d + (p + 1) * LANES]
                    v = qkv_b[layer, rs, 2 * d + p * LANES : 2 * d + (p + 1) * LANES].astype(F32)
                    q2 = split_rows(q, half_mask)
                    q_hi = q2.astype(BF)
                    q_lo = (q2 - q_hi.astype(F32)).astype(BF)
                    k_hi = k.astype(BF)
                    k_lo = (k - k_hi.astype(F32)).astype(BF)
                    scores = mm_nt(
                        jnp.concatenate([q_hi, q_lo], 1), jnp.concatenate([k_hi, k_hi], 1)
                    ) + mm_nt(q_hi, k_lo)
                    scores = jnp.where(block_mask, scores, -1e30)
                    top = jnp.max(scores, axis=1, keepdims=True)
                    e = jnp.exp(scores - top)
                    weight = (e / jnp.sum(e, axis=1, keepdims=True)).astype(BF)
                    prob[layer, g * pairs + p] = weight
                    o = mm(
                        jnp.concatenate([weight[:LANES], weight[LANES:]], 1),
                        split_rows(v, half_mask).astype(BF),
                    )
                    c_o[layer, rs, p * LANES : (p + 1) * LANES] = o.astype(BF)
            y = x_ref[...] + mm(c_o[layer], w_in[layer, :, 3 * d : 4 * d])
            y_ref[...] = y
            normed, scale = norm_forward(y)
            u2 = normed.astype(BF)
            c_u2[layer] = u2
            r2[layer] = scale
            for part in range(ff // chunk):
                cs = slice(part * chunk, (part + 1) * chunk)
                pre = mm(u2, w_in[layer, :, 4 * d + part * chunk : 4 * d + (part + 1) * chunk])
                square = pre * pre
                t = jnp.tanh(GELU_A * pre * (1.0 + GELU_B * square))
                half = 0.5 * (1.0 + t)
                c_h[layer, :, cs] = (pre * half).astype(BF)
                slope = half + 0.5 * pre * (1.0 - t * t) * (GELU_A * (1.0 + 3.0 * GELU_B * square))
                gp[layer, :, cs] = slope.astype(BF)
            x_ref[...] = y_ref[...] + mm(c_h[layer], w_down[layer])

            @pl.when(layer == 0)
            def _():
                cut = x_ref[...].astype(BF).astype(F32)
                x_ref[...] = jnp.where(row_slot < filled, cut, 0.0)

            return carry

        lax.fori_loop(0, layers, forward, 0)

        pooled = jnp.mean(x_ref[...].reshape(images, tok, d), axis=1)
        pnorm, pscale = norm_forward(pooled)
        pb = pnorm.astype(BF)
        here = lax.broadcasted_iota(jnp.int32, classifier.shape, 1) == shard
        weights_cls = jnp.sum(jnp.where(here, classifier[...].astype(F32), 0.0), axis=1).astype(BF)
        logits = mm_nt(pb, weights_cls)
        image = lax.broadcasted_iota(jnp.int32, (images, 1), 0)
        label = jnp.zeros((images, 1), jnp.int32)
        for n in range(images):
            k, i = n // per_image, n % per_image
            value = labels[slot[k] * cfg["img"] + rank * per_image + i]
            label = jnp.where(image == n, value, label)
        full = (image // per_image < filled).astype(F32)
        hot = (lax.broadcasted_iota(jnp.int32, (images, classes), 1) == label).astype(F32)
        top = jnp.max(logits, axis=1, keepdims=True)
        e = jnp.exp(logits - top)
        total = jnp.sum(e, axis=1, keepdims=True)
        picked = jnp.sum(hot * logits, axis=1, keepdims=True)
        loss = (jnp.log(total) + top - picked) * full
        diagonal = lax.broadcasted_iota(jnp.int32, (images, images), 1) == image
        losses[...] = jnp.sum(jnp.where(diagonal, loss, 0.0), axis=0, keepdims=True)
        dlogits = ((e / total - hot) * full).astype(BF)
        dcls[...] = mm_tn(dlogits, pb)
        dpb = mm(dlogits, weights_cls).astype(BF).astype(F32)
        dpool = norm_backward(dpb, pnorm, pscale) * (1.0 / tok)
        x_ref[...] = jnp.broadcast_to(dpool[:, None, :], (images, tok, d)).reshape(rows, d)

        def backward(step, carry):
            layer = layers - 1 - step
            dout = x_ref[...]
            dob = dout.astype(BF)
            c_dout[layer] = dob
            for part in range(ff // chunk):
                cs = slice(part * chunk, (part + 1) * chunk)
                dh = mm_nt(dob, w_down[layer, cs]).astype(BF).astype(F32)
                c_dpre[layer, :, cs] = (dh * gp[layer, :, cs].astype(F32)).astype(BF)
            du2 = mm_nt(c_dpre[layer], w_in[layer, :, 4 * d :]).astype(BF).astype(F32)
            dy = x_ref[...] + norm_backward(du2, c_u2[layer].astype(F32), r2[layer])
            y_ref[...] = dy
            dyb = dy.astype(BF)
            c_dy[layer] = dyb
            do = mm_nt(dyb, w_in[layer, :, 3 * d : 4 * d]).astype(BF).astype(F32)
            head_dim = d // HEADS
            for g in range(halves):
                rs = slice(g * LANES, (g + 1) * LANES)
                for p in range(pairs):
                    ls = slice(p * LANES, (p + 1) * LANES)
                    d2 = split_rows(do[rs, ls], half_mask).astype(BF)
                    q = qkv_b[layer, rs, p * LANES : (p + 1) * LANES].astype(F32)
                    k = qkv_b[layer, rs, d + p * LANES : d + (p + 1) * LANES].astype(F32)
                    v = qkv_b[layer, rs, 2 * d + p * LANES : 2 * d + (p + 1) * LANES]
                    weight = prob[layer, g * pairs + p]
                    wide = weight.astype(F32)
                    dprob = mm_nt(d2, v)
                    mixed = wide * dprob
                    dscore = mixed - wide * jnp.sum(mixed, axis=1, keepdims=True)
                    dscore = (dscore * (1.0 / math.sqrt(head_dim))).astype(BF)
                    dv = mm_tn(weight, d2)
                    dq = mm(
                        jnp.concatenate([dscore[:LANES], dscore[LANES:]], 1),
                        split_rows(k, half_mask).astype(BF),
                    )
                    dk = mm_tn(dscore, split_rows(q, half_mask).astype(BF))
                    c_dqkv[layer, rs, p * LANES : (p + 1) * LANES] = dq.astype(BF)
                    c_dqkv[layer, rs, d + p * LANES : d + (p + 1) * LANES] = dk.astype(BF)
                    c_dqkv[layer, rs, 2 * d + p * LANES : 2 * d + (p + 1) * LANES] = dv.astype(BF)
            du = mm_nt(c_dqkv[layer], w_in[layer, :, : 3 * d]).astype(BF).astype(F32)
            dx = y_ref[...] + norm_backward(du, c_u[layer].astype(F32), r1[layer])
            x_ref[...] = dx

            @pl.when(layer == 1)
            def _():
                x_ref[...] = x_ref[...].astype(BF).astype(F32)

            for which in range(1, layers):

                @pl.when(layer == which)
                def _(which=which):
                    for copy in saved_copies(which):
                        copy.start()

            return carry

        lax.fori_loop(0, layers, backward, 0)

        chip = me // 2

        def emit(values, at):
            for n in sorted(values)[::2]:
                own = jnp.where(core == 0, values[n], values[n + 1])
                other = jnp.where(core == 0, values[n + 1], values[n])
                keep[slot_of_chip(chip ^ (n // 2), core, bits), at] = own.astype(BF)
                send[slot_of_chip(chip ^ (n // 2), 1 - core, bits), at] = other.astype(BF)

        def emit_columns(first, cot, act):
            value = mm_tn(cot, act)
            count = value.shape[0] // cin
            base = first // cin
            emit(
                {base + i: value[i * cin : (i + 1) * cin] for i in range(count)},
                slice(0, cin),
            )

        width = members * ROWS16
        column = lax.broadcasted_iota(jnp.int32, (d, width), 1)
        row = lax.broadcasted_iota(jnp.int32, (d, width), 0)
        inner = column % ROWS16
        sel = ((inner < dpc) & (row == (column // ROWS16) * dpc + inner)).astype(BF)
        dob_pad[...] = mm(c_dout[0], sel).astype(BF)
        for part in range(ff // d):
            value = mm_tn(dob_pad[...], c_h[0, :, part * d : (part + 1) * d])
            emit(
                {n: value[n * ROWS16 : (n + 1) * ROWS16] for n in range(members)},
                slice(cin_pad + part * ROWS16, cin_pad + (part + 1) * ROWS16),
            )
        copies = grad_copies(0, cin_pad, (ff // d) * ROWS16)
        for copy in copies:
            copy.start()
        for part in range(3):
            emit_columns(part * d, c_dqkv[0, :, part * d : (part + 1) * d], c_u[0])
        emit_columns(3 * d, c_dy[0], c_o[0])
        for part in range(ff // d):
            emit_columns(4 * d + part * d, c_dpre[0, :, part * d : (part + 1) * d], c_u2[0])

        copies += grad_copies(1, 0, cin_pad)
        for copy in copies[2:]:
            copy.start()
        dob_pad[...] = mm(x_ref[...].astype(BF), sel).astype(BF)
        value = jnp.concatenate([mm(pcat[...], dob_pad[...]), jnp.zeros((d - patch - tok, width), F32)], 0).T
        base = cin_pad + (ff // d) * ROWS16
        emit(
            {n: value[n * ROWS16 : (n + 1) * ROWS16] for n in range(members)},
            slice(base, base + ROWS16),
        )
        copies += grad_copies(2, base, ROWS16)
        for copy in copies[4:]:
            copy.start()
        for layer in range(1, layers):
            copies += saved_copies(layer)
        for copy in copies:
            copy.wait()

    height = cin_pad + (ff // d) * ROWS16 + ROWS16
    cfg["height"] = height
    wide = 4 * d + ff
    saved = [d, d, d, ff, 3 * d, d, ff, d]
    out_shape = [
        jax.ShapeDtypeStruct((1, images), F32),
        jax.ShapeDtypeStruct((classes, d), F32),
        jax.ShapeDtypeStruct((chips, height, d), BF),
        jax.ShapeDtypeStruct((chips, height, d), BF),
    ] + [jax.ShapeDtypeStruct((layers - 1, rows, w), BF) for w in saved]
    any_spec = pl.BlockSpec(memory_space=pl.ANY)
    smem = pl.BlockSpec(memory_space=pltpu.SMEM)
    vmem = pl.BlockSpec(memory_space=pltpu.VMEM)
    n_sems = 2 + (layers - 1) * 2 * group + capacity + (layers - 1) * 8 + 6
    scratch = [
        pltpu.VMEM((layers, d, wide), BF),
        pltpu.VMEM((layers, ff, d), BF),
        pltpu.VMEM((capacity, packed, LANES), BF),
        pltpu.SMEM((capacity,), jnp.int32),
        pltpu.VMEM((rows, d), F32),
        pltpu.VMEM((rows, d), F32),
        pltpu.VMEM((rows, 3 * d), F32),
        pltpu.VMEM((layers, rows, 3 * d), BF),
        pltpu.VMEM((layers, halves * pairs, 2 * LANES, LANES), BF),
        pltpu.VMEM((layers, rows, ff), BF),
        pltpu.VMEM((layers, rows, 1), F32),
        pltpu.VMEM((layers, rows, 1), F32),
    ]
    scratch += [pltpu.VMEM((layers, rows, w), BF) for w in saved]
    scratch += [
        pltpu.VMEM((patch + tok, rows), BF),
        pltpu.VMEM((rows, members * ROWS16), BF),
        pltpu.VMEM((chips, height, d), BF),
        pltpu.VMEM((chips, height, d), BF),
        pltpu.SemaphoreType.DMA((n_sems,)),
    ]
    n_any = 2 * len(pieces)
    return pl.pallas_call(
        kernel,
        name="chain",
        in_specs=[smem, smem, any_spec, vmem, vmem, any_spec, any_spec]
        + [any_spec] * n_any
        + [vmem],
        out_specs=[vmem, vmem] + [any_spec] * (len(out_shape) - 2),
        out_shape=out_shape,
        scratch_shapes=scratch,
        compiler_params=pltpu.CompilerParams(vmem_limit_bytes=58 * 1024 * 1024),
    )


def make_pack(cfg):
    members, group, patch = cfg["members"], cfg["group"], cfg["patch"]
    packed, width = patch // group, LANES // group

    def kernel(patches, out):
        lane = lax.broadcasted_iota(jnp.int32, (packed, LANES), 1)
        parts = [patches[s * packed : (s + 1) * packed].astype(F32) for s in range(group)]
        for j in range(group):
            value = parts[0]
            for s in range(group):
                moved = pltpu.roll(parts[s], (width * (s - j)) % LANES, 1)
                value = jnp.where(lane // width == s, moved, value)
            value = value.astype(BF)
            for shard in range(members // group):
                out[shard * group + j] = value

    return pl.pallas_call(
        kernel, name="pack", out_shape=jax.ShapeDtypeStruct((members, packed, LANES), BF)
    )


def make_server_grads(cfg):
    d, ff, group, layers = cfg["d"], cfg["ff"], cfg["group"], cfg["layers"]
    rows_in, rows_down = d // group, ff // group
    wide = 4 * d + ff
    half = group // 2

    def kernel(u, o, u2, h, dqkv, dy, dpre, dout, k_in, s_in, k_down, s_down, t_in, t_down):
        rank = lax.axis_index("client") % group
        for part in range(3):
            t_in[:, part * d : (part + 1) * d] = mm_tn(u[...], dqkv[:, part * d : (part + 1) * d]).astype(BF)
        t_in[:, 3 * d : 4 * d] = mm_tn(o[...], dy[...]).astype(BF)
        for part in range(ff // d):
            cs = slice(part * d, (part + 1) * d)
            t_in[:, 4 * d + part * d : 4 * d + (part + 1) * d] = mm_tn(u2[...], dpre[:, cs]).astype(BF)
            t_down[cs] = mm_tn(h[:, cs], dout[...]).astype(BF)
        for p in range(group):
            owner = rank ^ p
            o_in, o_down = (k_in, k_down) if p < half else (s_in, s_down)
            o_in[p % half] = t_in[pl.ds(pl.multiple_of(owner * rows_in, rows_in), rows_in)]
            o_down[p % half] = t_down[pl.ds(pl.multiple_of(owner * rows_down, rows_down), rows_down)]

    rows = cfg["capacity"] * cfg["pr"]
    flops = 2 * rows * (d * wide + ff * d) * (layers - 1)
    saved = [d, d, d, ff, 3 * d, d, ff, d]
    in_block = pl.BlockSpec((half, None, rows_in, wide), lambda i: (0, i, 0, 0))
    down_block = pl.BlockSpec((half, None, rows_down, d), lambda i: (0, i, 0, 0))
    return pl.pallas_call(
        kernel,
        name="server_grads",
        grid=(layers - 1,),
        in_specs=[pl.BlockSpec((None, rows, w), lambda i: (i, 0, 0)) for w in saved],
        out_specs=[in_block, in_block, down_block, down_block],
        out_shape=[jax.ShapeDtypeStruct((half, layers - 1, rows_in, wide), BF)] * 2
        + [jax.ShapeDtypeStruct((half, layers - 1, rows_down, d), BF)] * 2,
        scratch_shapes=[pltpu.VMEM((d, wide), BF), pltpu.VMEM((ff, d), BF)],
        cost_estimate=pl.CostEstimate(flops=flops * 4, bytes_accessed=16 * 2**20, transcendentals=0),
        compiler_params=pltpu.CompilerParams(vmem_limit_bytes=48 * 1024 * 1024),
    )


def make_finish(cfg):
    d, ff, tok, patch = cfg["d"], cfg["ff"], cfg["tok"], cfg["patch"]
    members, cin, cin_pad, group = cfg["members"], cfg["cin"], cfg["cin_pad"], cfg["group"]
    classes = cfg["classes"]
    dpc, rows_in = d // members, d // group

    def kernel(a, b, cls, g_embed, g_pos, g_in, g_down, g_class):
        total = a[0].astype(F32) + b[0].astype(F32)
        g_in[...] = total[:cin]
        for part in range(ff // d):
            first = cin_pad + part * ROWS16
            g_down[:, part * d : (part + 1) * d] = total[first : first + dpc]
        first = cin_pad + (ff // d) * ROWS16
        g_embed[...] = total[first : first + dpc, :patch]
        g_pos[...] = total[first : first + dpc, patch : patch + tok]
        rank = lax.axis_index("client") % group
        value = cls[:, :rows_in]
        for r in range(1, group):
            value = jnp.where(rank == r, cls[:, r * rows_in : (r + 1) * rows_in], value)
        g_class[...] = value

    return pl.pallas_call(
        kernel,
        name="finish",
        out_shape=[
            jax.ShapeDtypeStruct((dpc, patch), F32),
            jax.ShapeDtypeStruct((dpc, tok), F32),
            jax.ShapeDtypeStruct((cin, d), F32),
            jax.ShapeDtypeStruct((dpc, ff), F32),
            jax.ShapeDtypeStruct((classes, rows_in), F32),
        ],
        compiler_params=pltpu.CompilerParams(vmem_limit_bytes=32 * 1024 * 1024),
    )


def swap_bit(block, bit):
    count = lax.axis_size("client")
    return lax.ppermute(block, "client", [(i, i ^ (1 << bit)) for i in range(count)])


def swap_by_core(block, even, odd):
    count = lax.axis_size("client")
    return lax.ppermute(
        block, "client", [(i, i ^ (1 << (even if i % 2 == 0 else odd))) for i in range(count)]
    )


def per_device(
    patches,
    labels,
    assign,
    patch_embed,
    positions,
    client_in,
    client_down,
    server_in,
    server_down,
    classifier,
):
    members = lax.axis_size("client")
    group = members // SHARDS
    group_bits = group.bit_length() - 1
    bits = members.bit_length() - 1
    patch, d = patch_embed.shape
    tok = positions.shape[0]
    ff = client_down.shape[0]
    img = labels.shape[0] // members
    layers = server_in.shape[0] + 1
    pr = patches.shape[0] // group
    rows_in, rows_down = server_in.shape[1], server_down.shape[1]
    cin = client_in.shape[1] // members
    capacity = SLOTS * group

    pieces, first = [1], [0]
    piece_in, piece_down = [server_in[None]], [server_down[None]]
    for bit in range(group_bits):
        whole_in = piece_in[0] if bit == 0 else jnp.concatenate(piece_in, 0)
        whole_down = piece_down[0] if bit == 0 else jnp.concatenate(piece_down, 0)
        piece_in.append(swap_bit(whole_in, bit))
        piece_down.append(swap_bit(whole_down, bit))
        first.append(1 << bit)
        pieces.append(1 << bit)

    cfg = dict(
        d=d,
        ff=ff,
        tok=tok,
        patch=patch,
        members=members,
        group=group,
        capacity=capacity,
        pr=pr,
        images=capacity * pr // tok,
        classes=classifier.shape[2],
        layers=layers,
        bits=bits,
        cin=cin,
        cin_pad=-(-cin // ROWS16) * ROWS16,
        pieces=pieces,
        first=first,
        packed=patch // group,
        img=img,
    )
    outgoing = make_pack(cfg)(patches.T)
    arrived = lax.all_to_all(outgoing, "client", split_axis=0, concat_axis=0, tiled=True)
    results = make_chain(cfg)(
        assign.reshape(-1),
        labels,
        arrived,
        patch_embed,
        positions,
        client_in,
        client_down,
        *piece_in,
        *piece_down,
        classifier.transpose(2, 0, 1),
    )
    losses, dcls, keep, send = results[:4]
    saved = results[4:]

    even, odd = stage_orders(bits)
    recv = swap_bit(send, 0)
    for step in range(bits - 1):
        half = keep.shape[0] // 2
        send = (keep[half:].astype(F32) + recv[half:].astype(F32)).astype(BF)
        keep = (keep[:half].astype(F32) + recv[:half].astype(F32)).astype(BF)
        recv = swap_by_core(send, even[step], odd[step])

    keep_in, send_in, keep_down, send_down = make_server_grads(cfg)(*saved)
    for bit in range(group_bits - 1, -1, -1):
        got_in = keep_in.astype(F32) + swap_bit(send_in, bit).astype(F32)
        got_down = keep_down.astype(F32) + swap_bit(send_down, bit).astype(F32)
        half = got_in.shape[0] // 2
        keep_in, send_in = got_in[:half], got_in[half:].astype(BF)
        keep_down, send_down = got_down[:half], got_down[half:].astype(BF)
    for bit in range(group_bits):
        dcls = dcls + swap_bit(dcls, bit)
    g_embed, g_pos, g_client_in, g_client_down, g_class = make_finish(cfg)(keep, recv, dcls)

    return (
        losses,
        g_embed.T,
        g_pos.T,
        g_client_in.T,
        g_client_down.T,
        got_in[0],
        got_down[0],
        g_class.T,
    )


def solution(mesh):
    in_specs = (
        P("client", None),
        P(),
        P(),
        P(),
        P(),
        P(),
        P(),
        P(None, "client", None),
        P(None, "client", None),
        P(),
    )
    out_specs = (
        P("client", None),
        P(None, "client"),
        P(None, "client"),
        P(None, "client"),
        P(None, "client"),
        P(None, "client", None),
        P(None, "client", None),
        P("client", None),
    )
    return jax.shard_map(
        per_device, mesh=mesh, in_specs=in_specs, out_specs=out_specs, check_vma=False
    )
```

```python
import math

import jax
import jax.numpy as jnp
from jax import lax
from jax.experimental import pallas as pl
from jax.experimental.pallas import tpu as pltpu
from jax.sharding import PartitionSpec as P

HEADS = 6
SHARDS = 16
SLOTS = 2
EPSILON = 1e-06
BF = jnp.bfloat16
F32 = jnp.float32
GELU_A = math.sqrt(2.0 / math.pi)
GELU_B = 0.044715
LANES = 128
ROWS16 = 16


def mm(a, b):
    return lax.dot_general(a, b, (((1,), (0,)), ((), ())), preferred_element_type=F32)


def mm_nt(a, b):
    return lax.dot_general(a, b, (((1,), (1,)), ((), ())), preferred_element_type=F32)


def mm_tn(a, b):
    return lax.dot_general(a, b, (((0,), (0,)), ((), ())), preferred_element_type=F32)


def norm_forward(x):
    centre = x - jnp.mean(x, axis=-1, keepdims=True)
    spread = jnp.mean(centre * centre, axis=-1, keepdims=True)
    scale = lax.rsqrt(spread + EPSILON)
    return centre * scale, scale


def norm_backward(grad, normed, scale):
    mean_grad = jnp.mean(grad, axis=-1, keepdims=True)
    mean_both = jnp.mean(grad * normed, axis=-1, keepdims=True)
    return scale * (grad - mean_grad - normed * mean_both)


PIECES = 3


def stage_order(bits, piece):
    if bits == 5:
        return ((1, 2, 3, 4), (2, 3, 1, 4), (3, 1, 2, 4))[piece]
    chip_bits = list(range(1, bits))
    turn = piece * max(1, len(chip_bits) // PIECES) % len(chip_bits)
    return tuple(chip_bits[turn:] + chip_bits[:turn])


def slot_of_chip(offset, bits, piece):
    value = 0
    for step, bit in enumerate(stage_order(bits, piece)):
        value = value | (((offset >> (bit - 1)) & 1) << (bits - 2 - step))
    return value


def compact(stacked, images, tok, lane_image):
    value = stacked[:tok]
    for i in range(1, images):
        value = jnp.where(lane_image == i, stacked[i * tok : (i + 1) * tok], value)
    return value


def expand(value, images, lane_image):
    return jnp.concatenate([jnp.where(lane_image == i, value, 0.0) for i in range(images)], axis=0).astype(BF)


def split_rows(x, mask):
    return jnp.concatenate([jnp.where(mask, x, 0.0), jnp.where(mask, 0.0, x)], axis=0)


def make_chain(cfg):
    d, ff, tok = cfg["d"], cfg["ff"], cfg["tok"]
    members, group, capacity, pr = cfg["members"], cfg["group"], cfg["capacity"], cfg["pr"]
    images, classes, patch = cfg["images"], cfg["classes"], cfg["patch"]
    layers, bits = cfg["layers"], cfg["bits"]
    rows = capacity * pr
    per_image = pr // tok
    rows_in, rows_down, pieces = d // group, ff // group, cfg["pieces"]
    cin = cfg["cin"]
    chips = members // 2
    halves = rows // LANES
    pairs = d // LANES
    dpc = d // members
    chunk = d
    heights = cfg["heights"]
    packed = cfg["packed"]

    def kernel(*refs):
        (assign, labels, arrived, embed_hbm, positions_hbm, client_in, client_down), refs = refs[:7], refs[7:]
        piece_in, refs = refs[: len(pieces)], refs[len(pieces) :]
        piece_down, refs = refs[: len(pieces)], refs[len(pieces) :]
        classifier_hbm, refs = refs[0], refs[1:]
        (losses, dcls), refs = refs[:2], refs[2:]
        grad_out, refs = refs[: 2 * PIECES], refs[2 * PIECES :]
        saved_out, refs = refs[:8], refs[8:]
        (w_in, w_down, slot, x_ref, y_ref, qkv_f, qkv_b, prob, gp, r1, r2), refs = refs[:11], refs[11:]
        (score, spread, dspread, embed, classifier), refs = refs[:5], refs[5:]
        saved_refs = refs[:8]
        (c_u, c_o, c_u2, c_h, c_dqkv, c_dy, c_dpre, c_dout, pcat, dob_pad), refs = refs[:10], refs[10:]
        grads, refs = refs[: 2 * PIECES], refs[2 * PIECES :]
        (sems,) = refs

        me = lax.axis_index("client")
        rank = me % group
        shard = me // group
        core = me % 2

        def weight_copies(layer, half):
            if layer == 0:
                wanted = ((pl.ds(0, 4 * d), 0),) if half == 0 else ((pl.ds(4 * d, ff), 1),)
                out = [
                    pltpu.make_async_copy(client_in.at[:, cols], w_in.at[0, :, cols], sems.at[sem])
                    for cols, sem in wanted
                ]
                if half == 1:
                    out.append(pltpu.make_async_copy(client_down, w_down.at[0], sems.at[2]))
                return out
            base = 3 + (layer - 1) * 2 * group + half
            sources, target, height = (
                (piece_in, w_in, rows_in) if half == 0 else (piece_down, w_down, rows_down)
            )
            out = []
            for source, start, count in zip(sources, cfg["first"], pieces):
                for inner in range(count):
                    index = start + inner
                    at = pl.ds(pl.multiple_of((rank ^ index) * height, height), height)
                    out.append(
                        pltpu.make_async_copy(
                            source.at[inner, layer - 1], target.at[layer, at], sems.at[base + 2 * index]
                        )
                    )
            return out

        first_other = 3 + (layers - 1) * 2 * group

        def saved_copies(layer):
            base = first_other + (layer - 1) * 8
            return [
                pltpu.make_async_copy(src.at[layer], dst.at[layer - 1], sems.at[base + i])
                for i, (src, dst) in enumerate(zip(saved_refs, saved_out))
            ]

        def grad_copies(piece):
            base = first_other + (layers - 1) * 8 + 2 * piece
            return [
                pltpu.make_async_copy(grads[2 * piece + i], grad_out[2 * piece + i], sems.at[base + i])
                for i in range(2)
            ]

        last_sem = first_other + (layers - 1) * 8 + 2 * PIECES
        small = [
            pltpu.make_async_copy(embed_hbm, embed.at[pl.ds(0, patch)], sems.at[last_sem]),
            pltpu.make_async_copy(positions_hbm, embed.at[pl.ds(patch, tok)], sems.at[last_sem + 1]),
        ]
        cls_copy = pltpu.make_async_copy(classifier_hbm, classifier, sems.at[last_sem + 2])
        for copy in small:
            copy.start()
        for half in range(2):
            for copy in weight_copies(0, half):
                copy.start()
        cls_copy.start()
        for k in range(capacity):
            slot[k] = 0

        def scan(c, count):
            hit = (assign[c] == shard) & (count < capacity)

            @pl.when(hit)
            def _():
                slot[count] = c

            return count + hit.astype(jnp.int32)

        filled = lax.fori_loop(0, members, scan, jnp.int32(0))
        half_mask = lax.broadcasted_iota(jnp.int32, (LANES, LANES), 1) < LANES // 2
        width_slot = LANES // group
        lane = lax.broadcasted_iota(jnp.int32, (packed, LANES), 1)
        for v in range(halves):
            blocks = [arrived[slot[v * group + t]].astype(F32) for t in range(group)]
            for part in range(group):
                value = blocks[0]
                for t in range(group):
                    moved = pltpu.roll(blocks[t], (width_slot * (t - part)) % LANES, 1)
                    value = jnp.where(lane // width_slot == t, moved, value)
                pcat[part * packed : (part + 1) * packed, v * LANES : (v + 1) * LANES] = value.astype(BF)
        token = lax.broadcasted_iota(jnp.int32, (tok, rows), 1) % tok
        pcat[patch:] = (token == lax.broadcasted_iota(jnp.int32, (tok, rows), 0)).astype(F32).astype(BF)
        for copy in small:
            copy.wait()
        x_ref[...] = mm_tn(pcat[...], embed[...])

        row_slot = lax.broadcasted_iota(jnp.int32, (rows, 1), 0) // pr
        group_images = LANES // tok
        lane_image = lax.broadcasted_iota(jnp.int32, (tok, LANES), 1) // tok

        def forward(layer, carry):
            for which in range(layers):

                @pl.when(layer == which)
                def _(which=which):
                    for copy in weight_copies(which, 0):
                        copy.wait()
                    if which == 0:
                        for later in range(1, layers):
                            for half in range(2):
                                for copy in weight_copies(later, half):
                                    copy.start()

            x = x_ref[...]
            normed, scale = norm_forward(x)
            u = normed.astype(BF)
            c_u[layer] = u
            r1[layer] = scale
            for part in range(3):
                value = mm(u, w_in[layer, :, part * d : (part + 1) * d])
                qkv_f[:, part * d : (part + 1) * d] = value
                qkv_b[layer, :, part * d : (part + 1) * d] = value.astype(BF)
            head_dim = d // HEADS
            tiles = [(g, p) for g in range(halves) for p in range(pairs)]
            for number, (g, p) in enumerate(tiles):
                rs = slice(g * LANES, (g + 1) * LANES)
                q = qkv_f[rs, p * LANES : (p + 1) * LANES] * (1.0 / math.sqrt(head_dim))
                k = qkv_f[rs, d + p * LANES : d + (p + 1) * LANES]
                k2 = split_rows(k, half_mask)
                k_hi = k2.astype(BF)
                k_lo = (k2 - k_hi.astype(F32)).astype(BF)
                q_hi = q.astype(BF)
                q_lo = (q - q_hi.astype(F32)).astype(BF)
                score[number] = mm_nt(
                    jnp.concatenate([k_hi, k_lo], 1), jnp.concatenate([q_hi, q_hi], 1)
                ) + mm_nt(k_hi, q_lo)
            for number in range(len(tiles)):
                for j in range(2):
                    part = compact(score[number, j * LANES : (j + 1) * LANES], group_images, tok, lane_image)
                    e = jnp.exp(part - jnp.max(part, axis=0, keepdims=True))
                    weight = e / jnp.sum(e, axis=0, keepdims=True)
                    prob[layer, 2 * number + j] = weight
                    spread[number, j * LANES : (j + 1) * LANES] = expand(weight, group_images, lane_image)
            for number, (g, p) in enumerate(tiles):
                rs = slice(g * LANES, (g + 1) * LANES)
                v = qkv_f[rs, 2 * d + p * LANES : 2 * d + (p + 1) * LANES]
                o = mm_tn(spread[number], split_rows(v, half_mask).astype(BF))
                c_o[layer, rs, p * LANES : (p + 1) * LANES] = o.astype(BF)
            for which in range(layers):

                @pl.when(layer == which)
                def _(which=which):
                    for copy in weight_copies(which, 1):
                        copy.wait()

            y = x_ref[...] + mm(c_o[layer], w_in[layer, :, 3 * d : 4 * d])
            y_ref[...] = y
            normed, scale = norm_forward(y)
            u2 = normed.astype(BF)
            c_u2[layer] = u2
            r2[layer] = scale
            for part in range(ff // chunk):
                cs = slice(part * chunk, (part + 1) * chunk)
                pre = mm(u2, w_in[layer, :, 4 * d + part * chunk : 4 * d + (part + 1) * chunk])
                square = pre * pre
                t = jnp.tanh(pre * (GELU_A + (GELU_A * GELU_B) * square))
                half = 0.5 * t + 0.5
                hidden = pre * half
                c_h[layer, :, cs] = hidden.astype(BF)
                slope = half + hidden * ((1.0 - half) * (2.0 * GELU_A + (6.0 * GELU_A * GELU_B) * square))
                gp[layer, :, cs] = slope.astype(BF)
            x_ref[...] = y_ref[...] + mm(c_h[layer], w_down[layer])

            @pl.when(layer == 0)
            def _():
                cut = x_ref[...].astype(BF).astype(F32)
                x_ref[...] = jnp.where(row_slot < filled, cut, 0.0)

            return carry

        lax.fori_loop(0, layers, forward, 0)

        cls_copy.wait()
        pooled = jnp.mean(x_ref[...].reshape(images, tok, d), axis=1)
        pnorm, pscale = norm_forward(pooled)
        pb = pnorm.astype(BF)
        here = lax.broadcasted_iota(jnp.int32, classifier.shape, 1) == shard
        weights_cls = jnp.sum(jnp.where(here, classifier[...].astype(F32), 0.0), axis=1).astype(BF)
        logits = mm_nt(pb, weights_cls)
        image = lax.broadcasted_iota(jnp.int32, (images, 1), 0)
        label = jnp.zeros((images, 1), jnp.int32)
        for n in range(images):
            k, i = n // per_image, n % per_image
            value = labels[slot[k] * cfg["img"] + rank * per_image + i]
            label = jnp.where(image == n, value, label)
        full = (image // per_image < filled).astype(F32)
        hot = (lax.broadcasted_iota(jnp.int32, (images, classes), 1) == label).astype(F32)
        top = jnp.max(logits, axis=1, keepdims=True)
        e = jnp.exp(logits - top)
        total = jnp.sum(e, axis=1, keepdims=True)
        picked = jnp.sum(hot * logits, axis=1, keepdims=True)
        loss = (jnp.log(total) + top - picked) * full
        diagonal = lax.broadcasted_iota(jnp.int32, (images, images), 1) == image
        losses[...] = jnp.sum(jnp.where(diagonal, loss, 0.0), axis=0, keepdims=True)
        dlogits = ((e / total - hot) * full).astype(BF)
        dcls[...] = mm_tn(dlogits, pb)
        dpb = mm(dlogits, weights_cls).astype(BF).astype(F32)
        dpool = norm_backward(dpb, pnorm, pscale) * (1.0 / tok)
        x_ref[...] = jnp.broadcast_to(dpool[:, None, :], (images, tok, d)).reshape(rows, d)

        def backward(step, carry):
            layer = layers - 1 - step
            dout = x_ref[...]
            dob = dout.astype(BF)
            c_dout[layer] = dob
            for part in range(ff // chunk):
                cs = slice(part * chunk, (part + 1) * chunk)
                dh = mm_nt(dob, w_down[layer, cs]).astype(BF).astype(F32)
                c_dpre[layer, :, cs] = (dh * gp[layer, :, cs].astype(F32)).astype(BF)
            du2 = mm_nt(c_dpre[layer], w_in[layer, :, 4 * d :]).astype(BF).astype(F32)
            dy = x_ref[...] + norm_backward(du2, c_u2[layer].astype(F32), r2[layer])
            y_ref[...] = dy
            dyb = dy.astype(BF)
            c_dy[layer] = dyb
            do = mm_nt(dyb, w_in[layer, :, 3 * d : 4 * d]).astype(BF)
            head_dim = d // HEADS
            tiles = [(g, p) for g in range(halves) for p in range(pairs)]
            qkv_f[:, :d] = do.astype(F32)
            for number, (g, p) in enumerate(tiles):
                rs, ls = slice(g * LANES, (g + 1) * LANES), slice(p * LANES, (p + 1) * LANES)
                v = qkv_b[layer, rs, 2 * d + p * LANES : 2 * d + (p + 1) * LANES].astype(F32)
                score[number] = mm_nt(split_rows(v, half_mask).astype(BF), qkv_f[rs, ls].astype(BF))
            for number in range(len(tiles)):
                for j in range(2):
                    weight = prob[layer, 2 * number + j]
                    part = compact(score[number, j * LANES : (j + 1) * LANES], group_images, tok, lane_image)
                    mixed = weight * part
                    dscore = mixed - weight * jnp.sum(mixed, axis=0, keepdims=True)
                    spread[number, j * LANES : (j + 1) * LANES] = expand(weight, group_images, lane_image)
                    dspread[number, j * LANES : (j + 1) * LANES] = expand(
                        dscore * (1.0 / math.sqrt(head_dim)), group_images, lane_image
                    )
            for number, (g, p) in enumerate(tiles):
                rs, ls = slice(g * LANES, (g + 1) * LANES), slice(p * LANES, (p + 1) * LANES)
                d2 = split_rows(qkv_f[rs, ls], half_mask).astype(BF)
                q = qkv_b[layer, rs, p * LANES : (p + 1) * LANES].astype(F32)
                k = qkv_b[layer, rs, d + p * LANES : d + (p + 1) * LANES].astype(F32)
                wide = jnp.concatenate([spread[number, :LANES], spread[number, LANES:]], 1)
                dwide = jnp.concatenate([dspread[number, :LANES], dspread[number, LANES:]], 1)
                dv = mm(wide, d2)
                dk = mm(dwide, split_rows(q, half_mask).astype(BF))
                dq = mm_tn(dspread[number], split_rows(k, half_mask).astype(BF))
                c_dqkv[layer, rs, p * LANES : (p + 1) * LANES] = dq.astype(BF)
                c_dqkv[layer, rs, d + p * LANES : d + (p + 1) * LANES] = dk.astype(BF)
                c_dqkv[layer, rs, 2 * d + p * LANES : 2 * d + (p + 1) * LANES] = dv.astype(BF)
            du = mm_nt(c_dqkv[layer], w_in[layer, :, : 3 * d]).astype(BF).astype(F32)
            dx = y_ref[...] + norm_backward(du, c_u[layer].astype(F32), r1[layer])
            x_ref[...] = dx

            @pl.when(layer == 1)
            def _():
                x_ref[...] = x_ref[...].astype(BF).astype(F32)

            for which in range(1, layers):

                @pl.when(layer == which)
                def _(which=which):
                    for copy in saved_copies(which):
                        copy.start()

            return carry

        lax.fori_loop(0, layers, backward, 0)

        chip = me // 2

        def emit(values, piece, at):
            for n in sorted(values)[::2]:
                own = jnp.where(core == 0, values[n], values[n + 1])
                other = jnp.where(core == 0, values[n + 1], values[n])
                place = slot_of_chip(chip ^ (n // 2), bits, piece)
                grads[2 * piece][place, at] = own.astype(BF)
                grads[2 * piece + 1][place, at] = other.astype(BF)

        copies = []
        for layer in range(1, layers):
            copies += saved_copies(layer)
        cut_at = heights[0]

        def emit_columns(first, cot, act):
            value = mm_tn(cot, act)
            count = value.shape[0] // cin
            base = first // cin
            for piece, low, high in ((0, 0, cut_at), (1, cut_at, cin)):
                emit(
                    {base + i: value[i * cin + low : i * cin + high] for i in range(count)},
                    piece,
                    slice(0, high - low),
                )

        for part in range(3):
            emit_columns(part * d, c_dqkv[0, :, part * d : (part + 1) * d], c_u[0])
        emit_columns(3 * d, c_dy[0], c_o[0])
        for part in range(ff // d):
            emit_columns(4 * d + part * d, c_dpre[0, :, part * d : (part + 1) * d], c_u2[0])
        for piece in range(2):
            for copy in grad_copies(piece):
                copy.start()
                copies.append(copy)

        width = members * ROWS16
        column = lax.broadcasted_iota(jnp.int32, (d, width), 1)
        row = lax.broadcasted_iota(jnp.int32, (d, width), 0)
        inner = column % ROWS16
        sel = ((inner < dpc) & (row == (column // ROWS16) * dpc + inner)).astype(BF)
        dob_pad[...] = mm(x_ref[...].astype(BF), sel).astype(BF)
        extra = jnp.concatenate([mm(pcat[...], dob_pad[...]), jnp.zeros((d - patch - tok, width), F32)], 0).T
        dob_pad[...] = mm(c_dout[0], sel).astype(BF)
        parts = ff // d
        share = -(-dpc // parts)
        out_row = lax.broadcasted_iota(jnp.int32, (width, d), 0) % ROWS16
        for part in range(parts):
            value = mm_tn(dob_pad[...], c_h[0, :, part * d : (part + 1) * d])
            moved = pltpu.roll(extra, (dpc - share * part) % width, 0)
            value = jnp.where((out_row >= dpc) & (out_row < dpc + share), moved, value)
            emit(
                {n: value[n * ROWS16 : (n + 1) * ROWS16] for n in range(members)},
                2,
                slice(part * ROWS16, (part + 1) * ROWS16),
            )
        for copy in grad_copies(2):
            copy.start()
            copies.append(copy)
        for copy in copies:
            copy.wait()

    wide = 4 * d + ff
    saved = [d, d, d, ff, 3 * d, d, ff, d]
    out_shape = [
        jax.ShapeDtypeStruct((1, images), F32),
        jax.ShapeDtypeStruct((classes, d), F32),
    ] + [jax.ShapeDtypeStruct((chips, height, d), BF) for height in heights for _ in range(2)]
    out_shape = out_shape + [jax.ShapeDtypeStruct((layers - 1, rows, w), BF) for w in saved]
    any_spec = pl.BlockSpec(memory_space=pl.ANY)
    hbm = pl.BlockSpec(memory_space=pltpu.HBM)
    smem = pl.BlockSpec(memory_space=pltpu.SMEM)
    vmem = pl.BlockSpec(memory_space=pltpu.VMEM)
    n_sems = 3 + (layers - 1) * 2 * group + (layers - 1) * 8 + 2 * PIECES + 3
    scratch = [
        pltpu.VMEM((layers, d, wide), BF),
        pltpu.VMEM((layers, ff, d), BF),
        pltpu.SMEM((capacity,), jnp.int32),
        pltpu.VMEM((rows, d), F32),
        pltpu.VMEM((rows, d), F32),
        pltpu.VMEM((rows, 3 * d), F32),
        pltpu.VMEM((layers, rows, 3 * d), BF),
        pltpu.VMEM((layers, halves * pairs * 2, tok, LANES), F32),
        pltpu.VMEM((layers, rows, ff), BF),
        pltpu.VMEM((layers, rows, 1), F32),
        pltpu.VMEM((layers, rows, 1), F32),
        pltpu.VMEM((halves * pairs, 2 * LANES, LANES), F32),
        pltpu.VMEM((halves * pairs, 2 * LANES, LANES), BF),
        pltpu.VMEM((halves * pairs, 2 * LANES, LANES), BF),
        pltpu.VMEM((patch + tok, d), BF),
        pltpu.VMEM((classes, members // group, d), BF),
    ]
    scratch += [pltpu.VMEM((layers, rows, w), BF) for w in saved]
    scratch += [
        pltpu.VMEM((patch + tok, rows), BF),
        pltpu.VMEM((rows, members * ROWS16), BF),
    ]
    scratch += [pltpu.VMEM((chips, height, d), BF) for height in heights for _ in range(2)]
    scratch += [
        pltpu.SemaphoreType.DMA((n_sems,)),
    ]
    return pl.pallas_call(
        kernel,
        name="chain",
        in_specs=[smem, smem, vmem] + [hbm] * (5 + 2 * len(pieces)),
        out_specs=[vmem, vmem] + [any_spec] * (len(out_shape) - 2),
        out_shape=out_shape,
        scratch_shapes=scratch,
        compiler_params=pltpu.CompilerParams(vmem_limit_bytes=cfg['vmem']),
    )


def make_pack(cfg):
    members, group, patch = cfg["members"], cfg["group"], cfg["patch"]
    packed, width = patch // group, LANES // group

    def kernel(patches, out):
        lane = lax.broadcasted_iota(jnp.int32, (packed, LANES), 1)
        parts = [patches[s * packed : (s + 1) * packed].astype(F32) for s in range(group)]
        for j in range(group):
            value = parts[0]
            for s in range(group):
                moved = pltpu.roll(parts[s], (width * (s - j)) % LANES, 1)
                value = jnp.where(lane // width == s, moved, value)
            value = value.astype(BF)
            for shard in range(members // group):
                out[shard * group + j] = value

    return pl.pallas_call(
        kernel, name="pack", out_shape=jax.ShapeDtypeStruct((members, packed, LANES), BF)
    )


def make_server_grads(cfg):
    d, ff, group, layers = cfg["d"], cfg["ff"], cfg["group"], cfg["layers"]
    rows_in, rows_down = d // group, ff // group
    wide = 4 * d + ff
    half = group // 2
    count = layers - 1
    rows = cfg["capacity"] * cfg["pr"]
    saved = [d, d, d, ff, 3 * d, d, ff, d]

    def kernel(*refs):
        sources, refs = refs[:8], refs[8:]
        k_in, s_in, k_down, s_down = refs[:4]
        local, t_in, t_down, sems = refs[4:12], refs[12], refs[13], refs[14]
        rank = lax.axis_index("client") % group

        def loads(layer):
            return [
                pltpu.make_async_copy(src.at[layer], dst.at[layer], sems.at[8 * layer + i])
                for i, (src, dst) in enumerate(zip(sources, local))
            ]

        def stores(layer):
            out = []
            for p in range(group):
                owner = rank ^ p
                o_in, o_down = (k_in, k_down) if p < half else (s_in, s_down)
                at_in = pl.ds(pl.multiple_of(owner * rows_in, rows_in), rows_in)
                at_down = pl.ds(pl.multiple_of(owner * rows_down, rows_down), rows_down)
                sem = 8 * count + 2 * (layer * group + p)
                out.append(pltpu.make_async_copy(t_in.at[layer, at_in], o_in.at[p % half, layer], sems.at[sem]))
                out.append(
                    pltpu.make_async_copy(t_down.at[layer, at_down], o_down.at[p % half, layer], sems.at[sem + 1])
                )
            return out

        for layer in range(count):
            for copy in loads(layer):
                copy.start()

        def compute(layer, carry):
            for which in range(count):

                @pl.when(layer == which)
                def _(which=which):
                    for copy in loads(which):
                        copy.wait()

            u, o, u2, h, dqkv, dy, dpre, dout = [ref.at[layer] for ref in local]
            for part in range(3):
                cs = slice(part * d, (part + 1) * d)
                t_in[layer, :, cs] = mm_tn(u[...], dqkv[:, cs]).astype(BF)
            t_in[layer, :, 3 * d : 4 * d] = mm_tn(o[...], dy[...]).astype(BF)
            for part in range(ff // d):
                cs = slice(part * d, (part + 1) * d)
                t_in[layer, :, 4 * d + part * d : 4 * d + (part + 1) * d] = mm_tn(u2[...], dpre[:, cs]).astype(BF)
                t_down[layer, cs] = mm_tn(h[:, cs], dout[...]).astype(BF)
            for which in range(count):

                @pl.when(layer == which)
                def _(which=which):
                    for copy in stores(which):
                        copy.start()

            return carry

        lax.fori_loop(0, count, compute, 0)
        for layer in range(count):
            for copy in stores(layer):
                copy.wait()

    flops = 2 * rows * (d * wide + ff * d) * count
    any_spec = pl.BlockSpec(memory_space=pl.ANY)
    return pl.pallas_call(
        kernel,
        name="server_grads",
        in_specs=[any_spec] * 8,
        out_specs=[any_spec] * 4,
        out_shape=[jax.ShapeDtypeStruct((half, count, rows_in, wide), BF)] * 2
        + [jax.ShapeDtypeStruct((half, count, rows_down, d), BF)] * 2,
        scratch_shapes=[pltpu.VMEM((count, rows, w), BF) for w in saved]
        + [
            pltpu.VMEM((count, d, wide), BF),
            pltpu.VMEM((count, ff, d), BF),
            pltpu.SemaphoreType.DMA((8 * count + 2 * count * group,)),
        ],
        cost_estimate=pl.CostEstimate(flops=flops * 2, bytes_accessed=16 * 2**20, transcendentals=0),
        compiler_params=pltpu.CompilerParams(vmem_limit_bytes=20 * 1024 * 1024),
    )


def make_finish(cfg):
    d, ff, tok, patch = cfg["d"], cfg["ff"], cfg["tok"], cfg["patch"]
    members, cin, group = cfg["members"], cfg["cin"], cfg["group"]
    classes = cfg["classes"]
    dpc, rows_in = d // members, d // group

    heights = cfg["heights"]
    parts = ff // d
    share = -(-dpc // parts)

    def kernel(a0, b0, a1, b1, a2, b2, cls, g_embed, g_pos, g_in, g_down, g_class):
        g_in[: heights[0]] = a0[0].astype(F32) + b0[0].astype(F32)
        g_in[heights[0] :] = (a1[0].astype(F32) + b1[0].astype(F32))[: cin - heights[0]]
        total = a2[0].astype(F32) + b2[0].astype(F32)
        extra = []
        for part in range(parts):
            block = total[part * ROWS16 : (part + 1) * ROWS16]
            g_down[:, part * d : (part + 1) * d] = block[:dpc]
            if share * part < dpc:
                extra.append(block[dpc : dpc + min(share, dpc - share * part)])
        extra = jnp.concatenate(extra, axis=0)
        g_embed[...] = extra[:, :patch]
        padded = jnp.concatenate([extra[:, patch : patch + tok], jnp.zeros((ROWS16 - dpc, tok), F32)], axis=0)
        g_pos[...] = padded.T[:, :dpc]
        rank = lax.axis_index("client") % group
        value = cls[:, :rows_in]
        for r in range(1, group):
            value = jnp.where(rank == r, cls[:, r * rows_in : (r + 1) * rows_in], value)
        g_class[...] = value

    return pl.pallas_call(
        kernel,
        name="finish",
        out_shape=[
            jax.ShapeDtypeStruct((dpc, patch), F32),
            jax.ShapeDtypeStruct((tok, dpc), F32),
            jax.ShapeDtypeStruct((cin, d), F32),
            jax.ShapeDtypeStruct((dpc, ff), F32),
            jax.ShapeDtypeStruct((classes, rows_in), F32),
        ],
        compiler_params=pltpu.CompilerParams(vmem_limit_bytes=32 * 1024 * 1024),
    )


def split_heights(cin, parts):
    first = cin // 2 if cin % (2 * ROWS16) == 0 else ROWS16
    return [first, -(-(cin - first) // ROWS16) * ROWS16, parts * ROWS16]


def swap_bit(block, bit):
    count = lax.axis_size("client")
    return lax.ppermute(block, "client", [(i, i ^ (1 << bit)) for i in range(count)])


def per_device(
    patches,
    labels,
    assign,
    patch_embed,
    positions,
    client_in,
    client_down,
    server_in,
    server_down,
    classifier,
):
    members = lax.axis_size("client")
    group = members // SHARDS
    group_bits = group.bit_length() - 1
    bits = members.bit_length() - 1
    patch, d = patch_embed.shape
    tok = positions.shape[0]
    ff = client_down.shape[0]
    img = labels.shape[0] // members
    layers = server_in.shape[0] + 1
    pr = patches.shape[0] // group
    rows_in, rows_down = server_in.shape[1], server_down.shape[1]
    cin = client_in.shape[1] // members
    capacity = SLOTS * group

    pieces, first = [1], [0]
    piece_in, piece_down = [server_in[None]], [server_down[None]]
    for bit in range(group_bits):
        whole_in = piece_in[0] if bit == 0 else jnp.concatenate(piece_in, 0)
        whole_down = piece_down[0] if bit == 0 else jnp.concatenate(piece_down, 0)
        piece_in.append(swap_bit(whole_in, bit))
        piece_down.append(swap_bit(whole_down, bit))
        first.append(1 << bit)
        pieces.append(1 << bit)

    cfg = dict(
        d=d,
        ff=ff,
        tok=tok,
        patch=patch,
        members=members,
        group=group,
        capacity=capacity,
        pr=pr,
        images=capacity * pr // tok,
        classes=classifier.shape[2],
        layers=layers,
        bits=bits,
        cin=cin,
        heights=split_heights(cin, ff // d),
        vmem=(44 if bits <= 5 else 58) * 2**20,
        pieces=pieces,
        first=first,
        packed=patch // group,
        img=img,
    )
    outgoing = make_pack(cfg)(patches.T)
    arrived = lax.all_to_all(outgoing, "client", split_axis=0, concat_axis=0, tiled=True)
    results = make_chain(cfg)(
        assign.reshape(-1),
        labels,
        arrived,
        patch_embed,
        positions,
        client_in,
        client_down,
        *piece_in,
        *piece_down,
        classifier.transpose(2, 0, 1),
    )
    losses, dcls = results[:2]
    grads = results[2 : 2 + 2 * PIECES]
    saved = results[2 + 2 * PIECES :]

    keeps, sends = list(grads[0::2]), list(grads[1::2])
    recvs = [swap_bit(send, 0) for send in sends]
    for step in range(bits - 1):
        for piece in range(PIECES):
            keep, recv = keeps[piece], recvs[piece]
            half = keep.shape[0] // 2
            sends[piece] = (keep[half:].astype(F32) + recv[half:].astype(F32)).astype(BF)
            keeps[piece] = (keep[:half].astype(F32) + recv[:half].astype(F32)).astype(BF)
        if step == 0:
            sends, saved = lax.optimization_barrier((sends, saved))
        if step == bits - 2:
            parts = make_server_grads(cfg)(*saved)
            keep_in, send_in, keep_down, send_down = parts
            for bit in range(group_bits - 1, -1, -1):
                recv_in, recv_down = swap_bit(send_in, bit), swap_bit(send_down, bit)
                if bit == 0:
                    sends, keep_in, keep_down = lax.optimization_barrier((sends, keep_in, keep_down))
                got_in = keep_in.astype(F32) + recv_in.astype(F32)
                got_down = keep_down.astype(F32) + recv_down.astype(F32)
                half = got_in.shape[0] // 2
                keep_in, send_in = got_in[:half], got_in[half:].astype(BF)
                keep_down, send_down = got_down[:half], got_down[half:].astype(BF)
        recvs = [swap_bit(sends[piece], stage_order(bits, piece)[step]) for piece in range(PIECES)]
    for bit in range(group_bits):
        dcls = dcls + swap_bit(dcls, bit)
    recvs, got_in, got_down = lax.optimization_barrier((recvs, got_in, got_down))
    g_embed, g_pos, g_client_in, g_client_down, g_class = make_finish(cfg)(
        *[array for pair in zip(keeps, recvs) for array in pair], dcls
    )

    return (
        losses,
        g_embed.T,
        g_pos,
        g_client_in.T,
        g_client_down.T,
        got_in[0],
        got_down[0],
        g_class.T,
    )


def solution(mesh):
    in_specs = (
        P("client", None),
        P(),
        P(),
        P(),
        P(),
        P(),
        P(),
        P(None, "client", None),
        P(None, "client", None),
        P(),
    )
    out_specs = (
        P("client", None),
        P(None, "client"),
        P(None, "client"),
        P(None, "client"),
        P(None, "client"),
        P(None, "client", None),
        P(None, "client", None),
        P("client", None),
    )
    return jax.shard_map(
        per_device, mesh=mesh, in_specs=in_specs, out_specs=out_specs, check_vma=False
    )
```

```python
import math

import jax
import jax.numpy as jnp
from jax import lax
from jax.experimental import pallas as pl
from jax.experimental.pallas import tpu as pltpu
from jax.sharding import PartitionSpec as P


HEADS = 6
SHARDS = 16
SLOTS = 2
EPSILON = 1e-06
BF = jnp.bfloat16
F32 = jnp.float32
GELU_A = math.sqrt(2.0 / math.pi)
GELU_B = 0.044715
LANES = 128
ROWS16 = 16


def mm(a, b):
    return lax.dot_general(a, b, (((1,), (0,)), ((), ())), preferred_element_type=F32)


def mm_nt(a, b):
    return lax.dot_general(a, b, (((1,), (1,)), ((), ())), preferred_element_type=F32)


def mm_tn(a, b):
    return lax.dot_general(a, b, (((0,), (0,)), ((), ())), preferred_element_type=F32)


def norm_forward(x):
    centre = x - jnp.mean(x, axis=-1, keepdims=True)
    spread = jnp.mean(centre * centre, axis=-1, keepdims=True)
    scale = lax.rsqrt(spread + EPSILON)
    return centre * scale, scale


def norm_backward(grad, normed, scale):
    mean_grad = jnp.mean(grad, axis=-1, keepdims=True)
    mean_both = jnp.mean(grad * normed, axis=-1, keepdims=True)
    return scale * (grad - mean_grad - normed * mean_both)


PIECES = 2


def stage_orders(bits, piece):
    if bits == 5:
        return (((1, 2, 3, 4), (2, 3, 1, 4)), ((3, 1, 2, 4), (3, 1, 2, 4)))[piece]
    *turning, last = range(1, bits)
    third = max(1, len(turning) // 3)
    turns = [tuple(turning[i * third :] + turning[: i * third]) + (last,) for i in range(3)]
    return ((turns[0], turns[1]), (turns[2], turns[2]))[piece]


def slot_of_chip(offset, core, bits, piece):
    def place(order):
        value = 0
        for step, bit in enumerate(order):
            value = value | (((offset >> (bit - 1)) & 1) << (bits - 2 - step))
        return value

    even, odd = stage_orders(bits, piece)
    return place(even) if even == odd else jnp.where(core == 0, place(even), place(odd))


def split_rows(x, mask):
    return jnp.concatenate([jnp.where(mask, x, 0.0), jnp.where(mask, 0.0, x)], axis=0)


def compact(stacked, images, tok, lane_image):
    value = stacked[:tok]
    for i in range(1, images):
        value = jnp.where(lane_image == i, stacked[i * tok : (i + 1) * tok], value)
    return value


def expand(value, images, lane_image):
    return jnp.concatenate([jnp.where(lane_image == i, value, 0.0) for i in range(images)], axis=0).astype(BF)


def make_chain(cfg):
    d, ff, tok = cfg["d"], cfg["ff"], cfg["tok"]
    members, group, capacity, pr = cfg["members"], cfg["group"], cfg["capacity"], cfg["pr"]
    images, classes, patch = cfg["images"], cfg["classes"], cfg["patch"]
    layers, bits = cfg["layers"], cfg["bits"]
    rows = capacity * pr
    per_image = pr // tok
    rows_in, rows_down, pieces = d // group, ff // group, cfg["pieces"]
    cin, cin_pad = cfg["cin"], cfg["cin_pad"]
    chips = members // 2
    halves = rows // LANES
    pairs = d // LANES
    dpc = d // members
    chunk = d
    heights = cfg["heights"]
    packed = cfg["packed"]

    def kernel(*refs):
        (assign, labels, arrived, embed_hbm, positions_hbm, client_in, client_down), refs = refs[:7], refs[7:]
        piece_in, refs = refs[: len(pieces)], refs[len(pieces) :]
        piece_down, refs = refs[: len(pieces)], refs[len(pieces) :]
        classifier_hbm, refs = refs[0], refs[1:]
        (losses, dcls), refs = refs[:2], refs[2:]
        grads, refs = refs[: 2 * PIECES], refs[2 * PIECES :]
        saved_out, refs = refs[:8], refs[8:]
        (w_in, w_down, slot, x_ref, y_ref, qkv_f, qkv_b, prob, gp, r1, r2), refs = refs[:11], refs[11:]
        (score, spread, dspread, embed, classifier), refs = refs[:5], refs[5:]
        saved_refs = refs[:8]
        (c_u, c_o, c_u2, c_h, c_dqkv, c_dy, c_dpre, c_dout, pcat, dob_pad), refs = refs[:10], refs[10:]
        (sems,) = refs

        me = lax.axis_index("client")
        rank = me % group
        shard = me // group
        core = me % 2

        def weight_copies(layer, half):
            if layer == 0:
                wanted = ((pl.ds(0, 4 * d), 0),) if half == 0 else ((pl.ds(4 * d, ff), 1),)
                out = [
                    pltpu.make_async_copy(client_in.at[:, cols], w_in.at[0, :, cols], sems.at[sem])
                    for cols, sem in wanted
                ]
                if half == 1:
                    out.append(pltpu.make_async_copy(client_down, w_down.at[0], sems.at[2]))
                return out
            base = 3 + (layer - 1) * 2 * group + half
            sources, target, height = (
                (piece_in, w_in, rows_in) if half == 0 else (piece_down, w_down, rows_down)
            )
            out = []
            for source, start, count in zip(sources, cfg["first"], pieces):
                for inner in range(count):
                    index = start + inner
                    at = pl.ds(pl.multiple_of((rank ^ index) * height, height), height)
                    out.append(
                        pltpu.make_async_copy(
                            source.at[inner, layer - 1], target.at[layer, at], sems.at[base + 2 * index]
                        )
                    )
            return out

        first_other = 3 + (layers - 1) * 2 * group

        def saved_copies(layer):
            base = first_other + (layer - 1) * 8
            return [
                pltpu.make_async_copy(src.at[layer], dst.at[layer - 1], sems.at[base + i])
                for i, (src, dst) in enumerate(zip(saved_refs, saved_out))
            ]

        last_sem = first_other + (layers - 1) * 8
        small = [
            pltpu.make_async_copy(embed_hbm, embed.at[pl.ds(0, patch)], sems.at[last_sem]),
            pltpu.make_async_copy(positions_hbm, embed.at[pl.ds(patch, tok)], sems.at[last_sem + 1]),
        ]
        cls_copy = pltpu.make_async_copy(classifier_hbm, classifier, sems.at[last_sem + 2])
        for copy in small:
            copy.start()
        for half in range(2):
            for copy in weight_copies(0, half):
                copy.start()
        cls_copy.start()
        for k in range(capacity):
            slot[k] = 0

        def scan(c, count):
            hit = (assign[c] == shard) & (count < capacity)

            @pl.when(hit)
            def _():
                slot[count] = c

            return count + hit.astype(jnp.int32)

        filled = lax.fori_loop(0, members, scan, jnp.int32(0))
        half_mask = lax.broadcasted_iota(jnp.int32, (LANES, LANES), 1) < LANES // 2
        width_slot = LANES // group
        lane = lax.broadcasted_iota(jnp.int32, (packed, LANES), 1)
        for v in range(halves):
            blocks = [arrived[slot[v * group + t]].astype(F32) for t in range(group)]
            for part in range(group):
                value = blocks[0]
                for t in range(group):
                    moved = pltpu.roll(blocks[t], (width_slot * (t - part)) % LANES, 1)
                    value = jnp.where(lane // width_slot == t, moved, value)
                pcat[part * packed : (part + 1) * packed, v * LANES : (v + 1) * LANES] = value.astype(BF)
        token = lax.broadcasted_iota(jnp.int32, (tok, rows), 1) % tok
        pcat[patch:] = (token == lax.broadcasted_iota(jnp.int32, (tok, rows), 0)).astype(F32).astype(BF)
        for copy in small:
            copy.wait()
        x_ref[...] = mm_tn(pcat[...], embed[...])

        row_slot = lax.broadcasted_iota(jnp.int32, (rows, 1), 0) // pr
        group_images = LANES // tok
        lane_image = lax.broadcasted_iota(jnp.int32, (tok, LANES), 1) // tok

        def forward(layer, carry):
            for which in range(layers):

                @pl.when(layer == which)
                def _(which=which):
                    for copy in weight_copies(which, 0):
                        copy.wait()
                    if which == 0:
                        for later in range(1, layers):
                            for half in range(2):
                                for copy in weight_copies(later, half):
                                    copy.start()

            x = x_ref[...]
            normed, scale = norm_forward(x)
            u = normed.astype(BF)
            c_u[layer] = u
            r1[layer] = scale
            for part in range(3):
                value = mm(u, w_in[layer, :, part * d : (part + 1) * d])
                qkv_f[:, part * d : (part + 1) * d] = value
                qkv_b[layer, :, part * d : (part + 1) * d] = value.astype(BF)
            head_dim = d // HEADS
            tiles = [(g, p) for g in range(halves) for p in range(pairs)]
            for number, (g, p) in enumerate(tiles):
                rs = slice(g * LANES, (g + 1) * LANES)
                q = qkv_f[rs, p * LANES : (p + 1) * LANES] * (1.0 / math.sqrt(head_dim))
                k = qkv_f[rs, d + p * LANES : d + (p + 1) * LANES]
                k2 = split_rows(k, half_mask)
                k_hi = k2.astype(BF)
                k_lo = (k2 - k_hi.astype(F32)).astype(BF)
                q_hi = q.astype(BF)
                q_lo = (q - q_hi.astype(F32)).astype(BF)
                score[number] = mm_nt(
                    jnp.concatenate([k_hi, k_lo], 1), jnp.concatenate([q_hi, q_hi], 1)
                ) + mm_nt(k_hi, q_lo)
            for number in range(len(tiles)):
                for j in range(2):
                    part = compact(score[number, j * LANES : (j + 1) * LANES], group_images, tok, lane_image)
                    e = jnp.exp(part - jnp.max(part, axis=0, keepdims=True))
                    weight = e / jnp.sum(e, axis=0, keepdims=True)
                    prob[layer, 2 * number + j] = weight
                    spread[number, j * LANES : (j + 1) * LANES] = expand(weight, group_images, lane_image)
            for number, (g, p) in enumerate(tiles):
                rs = slice(g * LANES, (g + 1) * LANES)
                v = qkv_f[rs, 2 * d + p * LANES : 2 * d + (p + 1) * LANES]
                o = mm_tn(spread[number], split_rows(v, half_mask).astype(BF))
                c_o[layer, rs, p * LANES : (p + 1) * LANES] = o.astype(BF)
            for which in range(layers):

                @pl.when(layer == which)
                def _(which=which):
                    for copy in weight_copies(which, 1):
                        copy.wait()

            y = x_ref[...] + mm(c_o[layer], w_in[layer, :, 3 * d : 4 * d])
            y_ref[...] = y
            normed, scale = norm_forward(y)
            u2 = normed.astype(BF)
            c_u2[layer] = u2
            r2[layer] = scale
            for part in range(ff // chunk):
                cs = slice(part * chunk, (part + 1) * chunk)
                pre = mm(u2, w_in[layer, :, 4 * d + part * chunk : 4 * d + (part + 1) * chunk])
                square = pre * pre
                t = jnp.tanh(pre * (GELU_A + (GELU_A * GELU_B) * square))
                half = 0.5 * t + 0.5
                hidden = pre * half
                c_h[layer, :, cs] = hidden.astype(BF)
                slope = half + hidden * ((1.0 - half) * (2.0 * GELU_A + (6.0 * GELU_A * GELU_B) * square))
                gp[layer, :, cs] = slope.astype(BF)
            x_ref[...] = y_ref[...] + mm(c_h[layer], w_down[layer])

            @pl.when(layer == 0)
            def _():
                cut = x_ref[...].astype(BF).astype(F32)
                x_ref[...] = jnp.where(row_slot < filled, cut, 0.0)

            return carry

        lax.fori_loop(0, layers, forward, 0)

        cls_copy.wait()
        pooled = jnp.mean(x_ref[...].reshape(images, tok, d), axis=1)
        pnorm, pscale = norm_forward(pooled)
        pb = pnorm.astype(BF)
        here = lax.broadcasted_iota(jnp.int32, classifier.shape, 1) == shard
        weights_cls = jnp.sum(jnp.where(here, classifier[...].astype(F32), 0.0), axis=1).astype(BF)
        logits = mm_nt(pb, weights_cls)
        image = lax.broadcasted_iota(jnp.int32, (images, 1), 0)
        label = jnp.zeros((images, 1), jnp.int32)
        for n in range(images):
            k, i = n // per_image, n % per_image
            value = labels[slot[k] * cfg["img"] + rank * per_image + i]
            label = jnp.where(image == n, value, label)
        full = (image // per_image < filled).astype(F32)
        hot = (lax.broadcasted_iota(jnp.int32, (images, classes), 1) == label).astype(F32)
        top = jnp.max(logits, axis=1, keepdims=True)
        e = jnp.exp(logits - top)
        total = jnp.sum(e, axis=1, keepdims=True)
        picked = jnp.sum(hot * logits, axis=1, keepdims=True)
        loss = (jnp.log(total) + top - picked) * full
        diagonal = lax.broadcasted_iota(jnp.int32, (images, images), 1) == image
        losses[...] = jnp.sum(jnp.where(diagonal, loss, 0.0), axis=0, keepdims=True)
        dlogits = ((e / total - hot) * full).astype(BF)
        dcls[...] = mm_tn(dlogits, pb)
        dpb = mm(dlogits, weights_cls).astype(BF).astype(F32)
        dpool = norm_backward(dpb, pnorm, pscale) * (1.0 / tok)
        x_ref[...] = jnp.broadcast_to(dpool[:, None, :], (images, tok, d)).reshape(rows, d)

        def backward(step, carry):
            layer = layers - 1 - step
            dout = x_ref[...]
            dob = dout.astype(BF)
            c_dout[layer] = dob
            for part in range(ff // chunk):
                cs = slice(part * chunk, (part + 1) * chunk)
                dh = mm_nt(dob, w_down[layer, cs]).astype(BF).astype(F32)
                c_dpre[layer, :, cs] = (dh * gp[layer, :, cs].astype(F32)).astype(BF)
            du2 = mm_nt(c_dpre[layer], w_in[layer, :, 4 * d :]).astype(BF).astype(F32)
            dy = x_ref[...] + norm_backward(du2, c_u2[layer].astype(F32), r2[layer])
            y_ref[...] = dy
            dyb = dy.astype(BF)
            c_dy[layer] = dyb
            do = mm_nt(dyb, w_in[layer, :, 3 * d : 4 * d]).astype(BF)
            head_dim = d // HEADS
            tiles = [(g, p) for g in range(halves) for p in range(pairs)]
            qkv_f[:, :d] = do.astype(F32)
            for number, (g, p) in enumerate(tiles):
                rs, ls = slice(g * LANES, (g + 1) * LANES), slice(p * LANES, (p + 1) * LANES)
                v = qkv_b[layer, rs, 2 * d + p * LANES : 2 * d + (p + 1) * LANES].astype(F32)
                score[number] = mm_nt(split_rows(v, half_mask).astype(BF), qkv_f[rs, ls].astype(BF))
            for number in range(len(tiles)):
                for j in range(2):
                    weight = prob[layer, 2 * number + j]
                    part = compact(score[number, j * LANES : (j + 1) * LANES], group_images, tok, lane_image)
                    mixed = weight * part
                    dscore = mixed - weight * jnp.sum(mixed, axis=0, keepdims=True)
                    spread[number, j * LANES : (j + 1) * LANES] = expand(weight, group_images, lane_image)
                    dspread[number, j * LANES : (j + 1) * LANES] = expand(
                        dscore * (1.0 / math.sqrt(head_dim)), group_images, lane_image
                    )
            for number, (g, p) in enumerate(tiles):
                rs, ls = slice(g * LANES, (g + 1) * LANES), slice(p * LANES, (p + 1) * LANES)
                d2 = split_rows(qkv_f[rs, ls], half_mask).astype(BF)
                q = qkv_b[layer, rs, p * LANES : (p + 1) * LANES].astype(F32)
                k = qkv_b[layer, rs, d + p * LANES : d + (p + 1) * LANES].astype(F32)
                wide = jnp.concatenate([spread[number, :LANES], spread[number, LANES:]], 1)
                dwide = jnp.concatenate([dspread[number, :LANES], dspread[number, LANES:]], 1)
                dv = mm(wide, d2)
                dk = mm(dwide, split_rows(q, half_mask).astype(BF))
                dq = mm_tn(dspread[number], split_rows(k, half_mask).astype(BF))
                c_dqkv[layer, rs, p * LANES : (p + 1) * LANES] = dq.astype(BF)
                c_dqkv[layer, rs, d + p * LANES : d + (p + 1) * LANES] = dk.astype(BF)
                c_dqkv[layer, rs, 2 * d + p * LANES : 2 * d + (p + 1) * LANES] = dv.astype(BF)
            du = mm_nt(c_dqkv[layer], w_in[layer, :, : 3 * d]).astype(BF).astype(F32)
            dx = y_ref[...] + norm_backward(du, c_u[layer].astype(F32), r1[layer])
            x_ref[...] = dx

            @pl.when(layer == 1)
            def _():
                x_ref[...] = x_ref[...].astype(BF).astype(F32)

            for which in range(1, layers):

                @pl.when(layer == which)
                def _(which=which):
                    for copy in saved_copies(which):
                        copy.start()

            return carry

        lax.fori_loop(0, layers, backward, 0)

        chip = me // 2

        def emit(values, piece, at):
            for n in sorted(values)[::2]:
                own = jnp.where(core == 0, values[n], values[n + 1])
                other = jnp.where(core == 0, values[n + 1], values[n])
                offset = chip ^ (n // 2)
                grads[2 * piece][slot_of_chip(offset, core, bits, piece), at] = own.astype(BF)
                grads[2 * piece + 1][slot_of_chip(offset, 1 - core, bits, piece), at] = other.astype(BF)

        copies = []
        for layer in range(1, layers):
            copies += saved_copies(layer)

        def emit_columns(first, cot, act):
            value = mm_tn(cot, act)
            count = value.shape[0] // cin
            base = first // cin
            emit({base + i: value[i * cin : (i + 1) * cin] for i in range(count)}, 0, slice(0, cin))

        for part in range(3):
            emit_columns(part * d, c_dqkv[0, :, part * d : (part + 1) * d], c_u[0])
        emit_columns(3 * d, c_dy[0], c_o[0])
        for part in range(ff // d):
            emit_columns(4 * d + part * d, c_dpre[0, :, part * d : (part + 1) * d], c_u2[0])
        width = members * ROWS16
        column = lax.broadcasted_iota(jnp.int32, (d, width), 1)
        row = lax.broadcasted_iota(jnp.int32, (d, width), 0)
        inner = column % ROWS16
        sel = ((inner < dpc) & (row == (column // ROWS16) * dpc + inner)).astype(BF)
        dob_pad[...] = mm(x_ref[...].astype(BF), sel).astype(BF)
        extra = jnp.concatenate([mm(pcat[...], dob_pad[...]), jnp.zeros((d - patch - tok, width), F32)], 0).T
        dob_pad[...] = mm(c_dout[0], sel).astype(BF)
        parts = ff // d
        share = -(-dpc // parts)
        out_row = lax.broadcasted_iota(jnp.int32, (width, d), 0) % ROWS16
        for part in range(parts):
            value = mm_tn(dob_pad[...], c_h[0, :, part * d : (part + 1) * d])
            moved = pltpu.roll(extra, (dpc - share * part) % width, 0)
            value = jnp.where((out_row >= dpc) & (out_row < dpc + share), moved, value)
            emit(
                {n: value[n * ROWS16 : (n + 1) * ROWS16] for n in range(members)},
                0 if part == 0 else 1,
                slice(cin_pad, cin_pad + ROWS16) if part == 0 else slice((part - 1) * ROWS16, part * ROWS16),
            )
        for copy in copies:
            copy.wait()

    wide = 4 * d + ff
    saved = [d, d, d, ff, 3 * d, d, ff, d]
    out_shape = [
        jax.ShapeDtypeStruct((1, images), F32),
        jax.ShapeDtypeStruct((classes, d), F32),
    ] + [jax.ShapeDtypeStruct((chips, height, d), BF) for height in heights for _ in range(2)]
    out_shape = out_shape + [pltpu.HBM((layers - 1, rows, w), BF) for w in saved]
    any_spec = pl.BlockSpec(memory_space=pl.ANY)
    hbm = pl.BlockSpec(memory_space=pltpu.HBM)
    smem = pl.BlockSpec(memory_space=pltpu.SMEM)
    vmem = pl.BlockSpec(memory_space=pltpu.VMEM)
    n_sems = 3 + (layers - 1) * 2 * group + (layers - 1) * 8 + 3
    scratch = [
        pltpu.VMEM((layers, d, wide), BF),
        pltpu.VMEM((layers, ff, d), BF),
        pltpu.SMEM((capacity,), jnp.int32),
        pltpu.VMEM((rows, d), F32),
        pltpu.VMEM((rows, d), F32),
        pltpu.VMEM((rows, 3 * d), F32),
        pltpu.VMEM((layers, rows, 3 * d), BF),
        pltpu.VMEM((layers, halves * pairs * 2, tok, LANES), F32),
        pltpu.VMEM((layers, rows, ff), BF),
        pltpu.VMEM((layers, rows, 1), F32),
        pltpu.VMEM((layers, rows, 1), F32),
        pltpu.VMEM((halves * pairs, 2 * LANES, LANES), F32),
        pltpu.VMEM((halves * pairs, 2 * LANES, LANES), BF),
        pltpu.VMEM((halves * pairs, 2 * LANES, LANES), BF),
        pltpu.VMEM((patch + tok, d), BF),
        pltpu.VMEM((classes, members // group, d), BF),
    ]
    scratch += [pltpu.VMEM((layers, rows, w), BF) for w in saved]
    scratch += [
        pltpu.VMEM((patch + tok, rows), BF),
        pltpu.VMEM((rows, members * ROWS16), BF),
    ]
    scratch += [
        pltpu.SemaphoreType.DMA((n_sems,)),
    ]
    return pl.pallas_call(
        kernel,
        name="chain",
        in_specs=[smem, smem, vmem] + [hbm] * (5 + 2 * len(pieces)),
        out_specs=[vmem] * (2 + 2 * PIECES) + [hbm] * (len(out_shape) - 2 - 2 * PIECES),
        out_shape=out_shape,
        scratch_shapes=scratch,
        compiler_params=pltpu.CompilerParams(vmem_limit_bytes=cfg['vmem']),
    )


def make_pack(cfg):
    members, group, patch = cfg["members"], cfg["group"], cfg["patch"]
    packed, width = patch // group, LANES // group

    def kernel(patches, out):
        lane = lax.broadcasted_iota(jnp.int32, (packed, LANES), 1)
        parts = [patches[s * packed : (s + 1) * packed].astype(F32) for s in range(group)]
        for j in range(group):
            value = parts[0]
            for s in range(group):
                moved = pltpu.roll(parts[s], (width * (s - j)) % LANES, 1)
                value = jnp.where(lane // width == s, moved, value)
            value = value.astype(BF)
            for shard in range(members // group):
                out[shard * group + j] = value

    return pl.pallas_call(
        kernel,
        name="pack",
        out_shape=jax.ShapeDtypeStruct((members, packed, LANES), BF),
    )


def make_stage(shapes):
    count = len(shapes)

    def kernel(*refs):
        sources, targets, sems = refs[:count], refs[count : 2 * count], refs[2 * count]
        copies = [pltpu.make_async_copy(sources[i], targets[i], sems.at[i]) for i in range(count)]
        for copy in copies:
            copy.start()
        for copy in copies:
            copy.wait()

    return pl.pallas_call(
        kernel,
        name="stage",
        in_specs=[pl.BlockSpec(memory_space=pl.ANY)] * count,
        out_specs=[pl.BlockSpec(memory_space=pltpu.HBM)] * count,
        out_shape=[pltpu.HBM(shape, BF) for shape in shapes],
        scratch_shapes=[pltpu.SemaphoreType.DMA((count,))],
    )


def make_server_grads(cfg):
    d, ff, group, layers = cfg["d"], cfg["ff"], cfg["group"], cfg["layers"]
    rows_in, rows_down = d // group, ff // group
    wide = 4 * d + ff
    half = group // 2
    count = layers - 1
    rows = cfg["capacity"] * cfg["pr"]
    saved = [d, d, d, ff, 3 * d, d, ff, d]

    def kernel(*refs):
        sources, refs = refs[:8], refs[8:]
        k_in, s_in, k_down, s_down = refs[:4]
        local, t_in, t_down, sems = refs[4:12], refs[12], refs[13], refs[14]
        rank = lax.axis_index("client") % group

        def loads(layer):
            return [
                pltpu.make_async_copy(src.at[layer], dst.at[layer], sems.at[8 * layer + i])
                for i, (src, dst) in enumerate(zip(sources, local))
            ]

        def stores(layer):
            out = []
            for p in range(group):
                owner = rank ^ p
                o_in, o_down = (k_in, k_down) if p < half else (s_in, s_down)
                at_in = pl.ds(pl.multiple_of(owner * rows_in, rows_in), rows_in)
                at_down = pl.ds(pl.multiple_of(owner * rows_down, rows_down), rows_down)
                sem = 8 * count + 2 * (layer * group + p)
                out.append(pltpu.make_async_copy(t_in.at[layer, at_in], o_in.at[p % half, layer], sems.at[sem]))
                out.append(
                    pltpu.make_async_copy(t_down.at[layer, at_down], o_down.at[p % half, layer], sems.at[sem + 1])
                )
            return out

        for layer in range(count):
            for copy in loads(layer):
                copy.start()

        def compute(layer, carry):
            for which in range(count):

                @pl.when(layer == which)
                def _(which=which):
                    for copy in loads(which):
                        copy.wait()

            u, o, u2, h, dqkv, dy, dpre, dout = [ref.at[layer] for ref in local]
            for part in range(3):
                cs = slice(part * d, (part + 1) * d)
                t_in[layer, :, cs] = mm_tn(u[...], dqkv[:, cs]).astype(BF)
            t_in[layer, :, 3 * d : 4 * d] = mm_tn(o[...], dy[...]).astype(BF)
            for part in range(ff // d):
                cs = slice(part * d, (part + 1) * d)
                t_in[layer, :, 4 * d + part * d : 4 * d + (part + 1) * d] = mm_tn(u2[...], dpre[:, cs]).astype(BF)
                t_down[layer, cs] = mm_tn(h[:, cs], dout[...]).astype(BF)
            for which in range(count):

                @pl.when(layer == which)
                def _(which=which):
                    for copy in stores(which):
                        copy.start()

            return carry

        lax.fori_loop(0, count, compute, 0)
        for layer in range(count):
            for copy in stores(layer):
                copy.wait()

    flops = 2 * rows * (d * wide + ff * d) * count
    any_spec = pl.BlockSpec(memory_space=pl.ANY)
    return pl.pallas_call(
        kernel,
        name="server_grads",
        in_specs=[any_spec] * 8,
        out_specs=[any_spec] * 4,
        out_shape=[jax.ShapeDtypeStruct((half, count, rows_in, wide), BF)] * 2
        + [jax.ShapeDtypeStruct((half, count, rows_down, d), BF)] * 2,
        scratch_shapes=[pltpu.VMEM((count, rows, w), BF) for w in saved]
        + [
            pltpu.VMEM((count, d, wide), BF),
            pltpu.VMEM((count, ff, d), BF),
            pltpu.SemaphoreType.DMA((8 * count + 2 * count * group,)),
        ],
        cost_estimate=pl.CostEstimate(flops=flops * 2, bytes_accessed=16 * 2**20, transcendentals=0),
        compiler_params=pltpu.CompilerParams(vmem_limit_bytes=20 * 1024 * 1024),
    )


def make_finish(cfg):
    d, ff, tok, patch = cfg["d"], cfg["ff"], cfg["tok"], cfg["patch"]
    members, cin, group = cfg["members"], cfg["cin"], cfg["group"]
    classes = cfg["classes"]
    dpc, rows_in = d // members, d // group

    heights, cin_pad = cfg["heights"], cfg["cin_pad"]
    parts = ff // d
    share = -(-dpc // parts)

    def kernel(a0, a1, b, cls, g_embed, g_pos, g_in, g_down, g_class):
        first = a0[0].astype(F32) + b[0, : heights[0]].astype(F32)
        g_in[...] = first[:cin]
        rest = a1[0].astype(F32) + b[0, heights[0] :].astype(F32)
        total = jnp.concatenate([first[cin_pad:], rest], axis=0)
        extra = []
        for part in range(parts):
            block = total[part * ROWS16 : (part + 1) * ROWS16]
            g_down[:, part * d : (part + 1) * d] = block[:dpc]
            if share * part < dpc:
                extra.append(block[dpc : dpc + min(share, dpc - share * part)])
        extra = jnp.concatenate(extra, axis=0)
        g_embed[...] = extra[:, :patch]
        padded = jnp.concatenate([extra[:, patch : patch + tok], jnp.zeros((ROWS16 - dpc, tok), F32)], axis=0)
        g_pos[...] = padded.T[:, :dpc]
        rank = lax.axis_index("client") % group
        value = cls[:, :rows_in]
        for r in range(1, group):
            value = jnp.where(rank == r, cls[:, r * rows_in : (r + 1) * rows_in], value)
        g_class[...] = value

    return pl.pallas_call(
        kernel,
        name="finish",
        out_shape=[
            jax.ShapeDtypeStruct((dpc, patch), F32),
            jax.ShapeDtypeStruct((tok, dpc), F32),
            jax.ShapeDtypeStruct((cin, d), F32),
            jax.ShapeDtypeStruct((dpc, ff), F32),
            jax.ShapeDtypeStruct((classes, rows_in), F32),
        ],
        compiler_params=pltpu.CompilerParams(vmem_limit_bytes=32 * 1024 * 1024),
    )


def swap_bit(block, bit):
    count = lax.axis_size("client")
    return lax.ppermute(block, "client", [(i, i ^ (1 << bit)) for i in range(count)])


def swap_by_core(block, even, odd):
    count = lax.axis_size("client")
    return lax.ppermute(
        block, "client", [(i, i ^ (1 << (even if i % 2 == 0 else odd))) for i in range(count)]
    )


def per_device(
    patches,
    labels,
    assign,
    patch_embed,
    positions,
    client_in,
    client_down,
    server_in,
    server_down,
    classifier,
):
    members = lax.axis_size("client")
    group = members // SHARDS
    group_bits = group.bit_length() - 1
    bits = members.bit_length() - 1
    patch, d = patch_embed.shape
    tok = positions.shape[0]
    ff = client_down.shape[0]
    img = labels.shape[0] // members
    layers = server_in.shape[0] + 1
    pr = patches.shape[0] // group
    cin = client_in.shape[1] // members
    capacity = SLOTS * group

    pieces, first = [1], [0]
    piece_in, piece_down = [server_in[None]], [server_down[None]]
    for bit in range(group_bits):
        whole_in = piece_in[0] if bit == 0 else jnp.concatenate(piece_in, 0)
        whole_down = piece_down[0] if bit == 0 else jnp.concatenate(piece_down, 0)
        piece_in.append(swap_bit(whole_in, bit))
        piece_down.append(swap_bit(whole_down, bit))
        first.append(1 << bit)
        pieces.append(1 << bit)

    cfg = dict(
        d=d,
        ff=ff,
        tok=tok,
        patch=patch,
        members=members,
        group=group,
        capacity=capacity,
        pr=pr,
        images=capacity * pr // tok,
        classes=classifier.shape[2],
        layers=layers,
        bits=bits,
        cin=cin,
        cin_pad=-(-cin // ROWS16) * ROWS16,
        heights=[-(-cin // ROWS16) * ROWS16 + ROWS16, (ff // d - 1) * ROWS16],
        vmem=(47 if bits <= 5 else 58) * 2**20,
        pieces=pieces,
        first=first,
        packed=patch // group,
        img=img,
    )
    others = piece_in[1:] + piece_down[1:]
    others = make_stage([array.shape for array in others])(*others)
    piece_in[1:], piece_down[1:] = others[:group_bits], others[group_bits:]

    outgoing = make_pack(cfg)(patches.T)
    arrived = lax.all_to_all(outgoing, "client", split_axis=0, concat_axis=0, tiled=True)
    results = make_chain(cfg)(
        assign.reshape(-1),
        labels,
        arrived,
        *[
            pltpu.with_memory_space_constraint(array, pltpu.HBM)
            for array in (
                patch_embed,
                positions,
                client_in,
                client_down,
                *piece_in,
                *piece_down,
                classifier.transpose(2, 0, 1),
            )
        ],
    )
    losses, dcls = results[:2]
    grads = results[2 : 2 + 2 * PIECES]
    saved = results[2 + 2 * PIECES :]

    keeps, sends = list(grads[0::2]), list(grads[1::2])
    for bit in range(group_bits):
        dcls = dcls + swap_bit(dcls, bit)
    recvs = [swap_bit(send, 0) for send in sends]
    for step in range(bits - 1):
        for piece in range(PIECES):
            keep, recv = keeps[piece], recvs[piece]
            half = keep.shape[0] // 2
            sends[piece] = (keep[half:].astype(F32) + recv[half:].astype(F32)).astype(BF)
            keeps[piece] = (keep[:half].astype(F32) + recv[:half].astype(F32)).astype(BF)
        if step == 0:
            sends, saved, dcls = lax.optimization_barrier((sends, saved, dcls))
        if step == bits - 2:
            parts = make_server_grads(cfg)(*[pltpu.with_memory_space_constraint(array, pltpu.HBM) for array in saved])
            keep_in, send_in, keep_down, send_down = parts
            for bit in range(group_bits - 1, -1, -1):
                recv_in, recv_down = swap_bit(send_in, bit), swap_bit(send_down, bit)
                if bit == 0:
                    sends, keep_in, keep_down = lax.optimization_barrier((sends, keep_in, keep_down))
                got_in = keep_in.astype(F32) + recv_in.astype(F32)
                got_down = keep_down.astype(F32) + recv_down.astype(F32)
                half = got_in.shape[0] // 2
                keep_in, send_in = got_in[:half], got_in[half:].astype(BF)
                keep_down, send_down = got_down[:half], got_down[half:].astype(BF)
        if step == bits - 2:
            recvs = swap_bit(jnp.concatenate(sends, axis=1), bits - 1)
            continue
        for piece in range(PIECES):
            even, odd = [order[step] for order in stage_orders(bits, piece)]
            recvs[piece] = swap_by_core(sends[piece], even, odd)
    recvs, got_in, got_down = lax.optimization_barrier((recvs, got_in, got_down))
    g_embed, g_pos, g_client_in, g_client_down, g_class = make_finish(cfg)(*keeps, recvs, dcls)

    return (
        losses,
        g_embed.T,
        g_pos,
        g_client_in.T,
        g_client_down.T,
        got_in[0],
        got_down[0],
        g_class.T,
    )


def solution(mesh):
    in_specs = (
        P("client", None),
        P(),
        P(),
        P(),
        P(),
        P(),
        P(),
        P(None, "client", None),
        P(None, "client", None),
        P(),
    )
    out_specs = (
        P("client", None),
        P(None, "client"),
        P(None, "client"),
        P(None, "client"),
        P(None, "client"),
        P(None, "client", None),
        P(None, "client", None),
        P("client", None),
    )
    return jax.shard_map(
        per_device, mesh=mesh, in_specs=in_specs, out_specs=out_specs, check_vma=False
    )
```

```python
import math

import jax
import jax.numpy as jnp
from jax import lax
from jax.experimental import pallas as pl
from jax.experimental.pallas import tpu as pltpu
from jax.sharding import PartitionSpec as P


HEADS = 6
SHARDS = 16
SLOTS = 2
EPSILON = 1e-06
BF = jnp.bfloat16
F32 = jnp.float32
GELU_A = math.sqrt(2.0 / math.pi)
GELU_B = 0.044715
LANES = 128
ROWS16 = 16


def mm(a, b):
    return lax.dot_general(a, b, (((1,), (0,)), ((), ())), preferred_element_type=F32)


def mm_nt(a, b):
    return lax.dot_general(a, b, (((1,), (1,)), ((), ())), preferred_element_type=F32)


def mm_tn(a, b):
    return lax.dot_general(a, b, (((0,), (0,)), ((), ())), preferred_element_type=F32)


def norm_forward(x):
    centre = x - jnp.mean(x, axis=-1, keepdims=True)
    spread = jnp.mean(centre * centre, axis=-1, keepdims=True)
    scale = lax.rsqrt(spread + EPSILON)
    return centre * scale, scale


def norm_backward(grad, normed, scale):
    mean_grad = jnp.mean(grad, axis=-1, keepdims=True)
    mean_both = jnp.mean(grad * normed, axis=-1, keepdims=True)
    return scale * (grad - mean_grad - normed * mean_both)


PIECES = 2


def stage_orders(bits, piece):
    if bits == 5:
        return (((1, 2, 3, 4), (2, 3, 1, 4)), ((3, 1, 2, 4), (3, 1, 2, 4)))[piece]
    *turning, last = range(1, bits)
    third = max(1, len(turning) // 3)
    turns = [tuple(turning[i * third :] + turning[: i * third]) + (last,) for i in range(3)]
    return ((turns[0], turns[1]), (turns[2], turns[2]))[piece]


def slot_of_chip(offset, core, bits, piece):
    def place(order):
        value = 0
        for step, bit in enumerate(order):
            value = value | (((offset >> (bit - 1)) & 1) << (bits - 2 - step))
        return value

    even, odd = stage_orders(bits, piece)
    return place(even) if even == odd else jnp.where(core == 0, place(even), place(odd))


def split_rows(x, mask):
    return jnp.concatenate([jnp.where(mask, x, 0.0), jnp.where(mask, 0.0, x)], axis=0)


def compact(stacked, images, tok, lane_image):
    value = stacked[:tok]
    for i in range(1, images):
        value = jnp.where(lane_image == i, stacked[i * tok : (i + 1) * tok], value)
    return value


def expand(value, images, lane_image):
    return jnp.concatenate([jnp.where(lane_image == i, value, 0.0) for i in range(images)], axis=0).astype(BF)


def make_chain(cfg):
    d, ff, tok = cfg["d"], cfg["ff"], cfg["tok"]
    members, group, capacity, pr = cfg["members"], cfg["group"], cfg["capacity"], cfg["pr"]
    images, classes, patch = cfg["images"], cfg["classes"], cfg["patch"]
    layers, bits = cfg["layers"], cfg["bits"]
    rows = capacity * pr
    per_image = pr // tok
    rows_in, rows_down, pieces = d // group, ff // group, cfg["pieces"]
    cin, cin_pad = cfg["cin"], cfg["cin_pad"]
    chips = members // 2
    halves = rows // LANES
    pairs = d // LANES
    dpc = d // members
    chunk = d
    heights = cfg["heights"]
    packed = cfg["packed"]

    def kernel(*refs):
        (assign, labels, arrived, embed_hbm, positions_hbm, client_in, client_down), refs = refs[:7], refs[7:]
        piece_in, refs = refs[: len(pieces)], refs[len(pieces) :]
        piece_down, refs = refs[: len(pieces)], refs[len(pieces) :]
        classifier_hbm, refs = refs[0], refs[1:]
        (losses, dcls), refs = refs[:2], refs[2:]
        grads, refs = refs[: 2 * PIECES], refs[2 * PIECES :]
        saved_out, refs = refs[:8], refs[8:]
        (w_in, w_down, slot, x_ref, y_ref, qkv_f, qkv_b, prob, gp, r1, r2), refs = refs[:11], refs[11:]
        (score, spread, dspread, embed, classifier), refs = refs[:5], refs[5:]
        saved_refs = refs[:8]
        (c_u, c_o, c_u2, c_h, c_dqkv, c_dy, c_dpre, c_dout, pcat, dob_pad), refs = refs[:10], refs[10:]
        (sems,) = refs

        me = lax.axis_index("client")
        rank = me % group
        shard = me // group
        core = me % 2

        def weight_copies(layer, half):
            if layer == 0:
                wanted = ((pl.ds(0, 4 * d), 0),) if half == 0 else ((pl.ds(4 * d, ff), 1),)
                out = [
                    pltpu.make_async_copy(client_in.at[:, cols], w_in.at[0, :, cols], sems.at[sem])
                    for cols, sem in wanted
                ]
                if half == 1:
                    out.append(pltpu.make_async_copy(client_down, w_down.at[0], sems.at[2]))
                return out
            base = 3 + (layer - 1) * 2 * group + half
            sources, target, height = (
                (piece_in, w_in, rows_in) if half == 0 else (piece_down, w_down, rows_down)
            )
            out = []
            for source, start, count in zip(sources, cfg["first"], pieces):
                for inner in range(count):
                    index = start + inner
                    at = pl.ds(pl.multiple_of((rank ^ index) * height, height), height)
                    out.append(
                        pltpu.make_async_copy(
                            source.at[inner, layer - 1], target.at[layer, at], sems.at[base + 2 * index]
                        )
                    )
            return out

        first_other = 3 + (layers - 1) * 2 * group

        def saved_copies(layer):
            base = first_other + (layer - 1) * 8
            return [
                pltpu.make_async_copy(src.at[layer], dst.at[layer - 1], sems.at[base + i])
                for i, (src, dst) in enumerate(zip(saved_refs, saved_out))
            ]

        last_sem = first_other + (layers - 1) * 8
        small = [
            pltpu.make_async_copy(embed_hbm, embed.at[pl.ds(0, patch)], sems.at[last_sem]),
            pltpu.make_async_copy(positions_hbm, embed.at[pl.ds(patch, tok)], sems.at[last_sem + 1]),
        ]
        cls_copy = pltpu.make_async_copy(classifier_hbm, classifier, sems.at[last_sem + 2])
        for copy in small:
            copy.start()
        for half in range(2):
            for copy in weight_copies(0, half):
                copy.start()
        cls_copy.start()
        for k in range(capacity):
            slot[k] = 0

        def scan(c, count):
            hit = (assign[c] == shard) & (count < capacity)

            @pl.when(hit)
            def _():
                slot[count] = c

            return count + hit.astype(jnp.int32)

        filled = lax.fori_loop(0, members, scan, jnp.int32(0))
        half_mask = lax.broadcasted_iota(jnp.int32, (LANES, LANES), 1) < LANES // 2
        width_slot = LANES // group
        lane = lax.broadcasted_iota(jnp.int32, (packed, LANES), 1)
        for v in range(halves):
            blocks = [arrived[slot[v * group + t]].astype(F32) for t in range(group)]
            for part in range(group):
                value = blocks[0]
                for t in range(group):
                    moved = pltpu.roll(blocks[t], (width_slot * (t - part)) % LANES, 1)
                    value = jnp.where(lane // width_slot == t, moved, value)
                pcat[part * packed : (part + 1) * packed, v * LANES : (v + 1) * LANES] = value.astype(BF)
        token = lax.broadcasted_iota(jnp.int32, (tok, rows), 1) % tok
        pcat[patch:] = (token == lax.broadcasted_iota(jnp.int32, (tok, rows), 0)).astype(F32).astype(BF)
        for copy in small:
            copy.wait()
        x_ref[...] = mm_tn(pcat[...], embed[...])

        row_slot = lax.broadcasted_iota(jnp.int32, (rows, 1), 0) // pr
        group_images = LANES // tok
        lane_image = lax.broadcasted_iota(jnp.int32, (tok, LANES), 1) // tok

        def forward(layer, carry):
            for which in range(layers):

                @pl.when(layer == which)
                def _(which=which):
                    for copy in weight_copies(which, 0):
                        copy.wait()
                    if which == 0:
                        for later in range(1, layers):
                            for half in range(2):
                                for copy in weight_copies(later, half):
                                    copy.start()

            x = x_ref[...]
            normed, scale = norm_forward(x)
            u = normed.astype(BF)
            c_u[layer] = u
            r1[layer] = scale
            for part in range(3):
                value = mm(u, w_in[layer, :, part * d : (part + 1) * d])
                qkv_f[:, part * d : (part + 1) * d] = value
                qkv_b[layer, :, part * d : (part + 1) * d] = value.astype(BF)
            head_dim = d // HEADS
            tiles = [(g, p) for g in range(halves) for p in range(pairs)]
            for number, (g, p) in enumerate(tiles):
                rs = slice(g * LANES, (g + 1) * LANES)
                q = qkv_f[rs, p * LANES : (p + 1) * LANES] * (1.0 / math.sqrt(head_dim))
                k = qkv_f[rs, d + p * LANES : d + (p + 1) * LANES]
                k2 = split_rows(k, half_mask)
                k_hi = k2.astype(BF)
                k_lo = (k2 - k_hi.astype(F32)).astype(BF)
                q_hi = q.astype(BF)
                q_lo = (q - q_hi.astype(F32)).astype(BF)
                score[number] = mm_nt(
                    jnp.concatenate([k_hi, k_lo], 1), jnp.concatenate([q_hi, q_hi], 1)
                ) + mm_nt(k_hi, q_lo)
            for number in range(len(tiles)):
                for j in range(2):
                    part = compact(score[number, j * LANES : (j + 1) * LANES], group_images, tok, lane_image)
                    e = jnp.exp(part - jnp.max(part, axis=0, keepdims=True))
                    weight = e / jnp.sum(e, axis=0, keepdims=True)
                    prob[layer, 2 * number + j] = weight
                    spread[number, j * LANES : (j + 1) * LANES] = expand(weight, group_images, lane_image)
            for number, (g, p) in enumerate(tiles):
                rs = slice(g * LANES, (g + 1) * LANES)
                v = qkv_f[rs, 2 * d + p * LANES : 2 * d + (p + 1) * LANES]
                o = mm_tn(spread[number], split_rows(v, half_mask).astype(BF))
                c_o[layer, rs, p * LANES : (p + 1) * LANES] = o.astype(BF)
            for which in range(layers):

                @pl.when(layer == which)
                def _(which=which):
                    for copy in weight_copies(which, 1):
                        copy.wait()

            y = x_ref[...] + mm(c_o[layer], w_in[layer, :, 3 * d : 4 * d])
            y_ref[...] = y
            normed, scale = norm_forward(y)
            u2 = normed.astype(BF)
            c_u2[layer] = u2
            r2[layer] = scale
            for part in range(ff // chunk):
                cs = slice(part * chunk, (part + 1) * chunk)
                pre = mm(u2, w_in[layer, :, 4 * d + part * chunk : 4 * d + (part + 1) * chunk])
                square = pre * pre
                t = jnp.tanh(pre * (GELU_A + (GELU_A * GELU_B) * square))
                half = 0.5 * t + 0.5
                hidden = pre * half
                c_h[layer, :, cs] = hidden.astype(BF)
                slope = half + hidden * ((1.0 - half) * (2.0 * GELU_A + (6.0 * GELU_A * GELU_B) * square))
                gp[layer, :, cs] = slope.astype(BF)
            x_ref[...] = y_ref[...] + mm(c_h[layer], w_down[layer])

            @pl.when(layer == 0)
            def _():
                cut = x_ref[...].astype(BF).astype(F32)
                x_ref[...] = jnp.where(row_slot < filled, cut, 0.0)

            return carry

        lax.fori_loop(0, layers, forward, 0)

        cls_copy.wait()
        pooled = jnp.mean(x_ref[...].reshape(images, tok, d), axis=1)
        pnorm, pscale = norm_forward(pooled)
        pb = pnorm.astype(BF)
        here = lax.broadcasted_iota(jnp.int32, classifier.shape, 1) == shard
        weights_cls = jnp.sum(jnp.where(here, classifier[...].astype(F32), 0.0), axis=1).astype(BF)
        logits = mm_nt(pb, weights_cls)
        image = lax.broadcasted_iota(jnp.int32, (images, 1), 0)
        label = jnp.zeros((images, 1), jnp.int32)
        for n in range(images):
            k, i = n // per_image, n % per_image
            value = labels[slot[k] * cfg["img"] + rank * per_image + i]
            label = jnp.where(image == n, value, label)
        full = (image // per_image < filled).astype(F32)
        hot = (lax.broadcasted_iota(jnp.int32, (images, classes), 1) == label).astype(F32)
        top = jnp.max(logits, axis=1, keepdims=True)
        e = jnp.exp(logits - top)
        total = jnp.sum(e, axis=1, keepdims=True)
        picked = jnp.sum(hot * logits, axis=1, keepdims=True)
        loss = (jnp.log(total) + top - picked) * full
        diagonal = lax.broadcasted_iota(jnp.int32, (images, images), 1) == image
        losses[...] = jnp.sum(jnp.where(diagonal, loss, 0.0), axis=0, keepdims=True)
        dlogits = ((e / total - hot) * full).astype(BF)
        dcls[...] = mm_tn(dlogits, pb)
        dpb = mm(dlogits, weights_cls).astype(BF).astype(F32)
        dpool = norm_backward(dpb, pnorm, pscale) * (1.0 / tok)
        x_ref[...] = jnp.broadcast_to(dpool[:, None, :], (images, tok, d)).reshape(rows, d)

        def backward(step, carry):
            layer = layers - 1 - step
            dout = x_ref[...]
            dob = dout.astype(BF)
            c_dout[layer] = dob
            for part in range(ff // chunk):
                cs = slice(part * chunk, (part + 1) * chunk)
                dh = mm_nt(dob, w_down[layer, cs]).astype(BF).astype(F32)
                c_dpre[layer, :, cs] = (dh * gp[layer, :, cs].astype(F32)).astype(BF)
            du2 = mm_nt(c_dpre[layer], w_in[layer, :, 4 * d :]).astype(BF).astype(F32)
            dy = x_ref[...] + norm_backward(du2, c_u2[layer].astype(F32), r2[layer])
            y_ref[...] = dy
            dyb = dy.astype(BF)
            c_dy[layer] = dyb
            do = mm_nt(dyb, w_in[layer, :, 3 * d : 4 * d]).astype(BF)
            head_dim = d // HEADS
            tiles = [(g, p) for g in range(halves) for p in range(pairs)]
            qkv_f[:, :d] = do.astype(F32)
            for number, (g, p) in enumerate(tiles):
                rs, ls = slice(g * LANES, (g + 1) * LANES), slice(p * LANES, (p + 1) * LANES)
                v = qkv_b[layer, rs, 2 * d + p * LANES : 2 * d + (p + 1) * LANES].astype(F32)
                score[number] = mm_nt(split_rows(v, half_mask).astype(BF), qkv_f[rs, ls].astype(BF))
            for number in range(len(tiles)):
                for j in range(2):
                    weight = prob[layer, 2 * number + j]
                    part = compact(score[number, j * LANES : (j + 1) * LANES], group_images, tok, lane_image)
                    mixed = weight * part
                    dscore = mixed - weight * jnp.sum(mixed, axis=0, keepdims=True)
                    spread[number, j * LANES : (j + 1) * LANES] = expand(weight, group_images, lane_image)
                    dspread[number, j * LANES : (j + 1) * LANES] = expand(
                        dscore * (1.0 / math.sqrt(head_dim)), group_images, lane_image
                    )
            for number, (g, p) in enumerate(tiles):
                rs, ls = slice(g * LANES, (g + 1) * LANES), slice(p * LANES, (p + 1) * LANES)
                d2 = split_rows(qkv_f[rs, ls], half_mask).astype(BF)
                q = qkv_b[layer, rs, p * LANES : (p + 1) * LANES].astype(F32)
                k = qkv_b[layer, rs, d + p * LANES : d + (p + 1) * LANES].astype(F32)
                wide = jnp.concatenate([spread[number, :LANES], spread[number, LANES:]], 1)
                dwide = jnp.concatenate([dspread[number, :LANES], dspread[number, LANES:]], 1)
                dv = mm(wide, d2)
                dk = mm(dwide, split_rows(q, half_mask).astype(BF))
                dq = mm_tn(dspread[number], split_rows(k, half_mask).astype(BF))
                c_dqkv[layer, rs, p * LANES : (p + 1) * LANES] = dq.astype(BF)
                c_dqkv[layer, rs, d + p * LANES : d + (p + 1) * LANES] = dk.astype(BF)
                c_dqkv[layer, rs, 2 * d + p * LANES : 2 * d + (p + 1) * LANES] = dv.astype(BF)
            du = mm_nt(c_dqkv[layer], w_in[layer, :, : 3 * d]).astype(BF).astype(F32)
            dx = y_ref[...] + norm_backward(du, c_u[layer].astype(F32), r1[layer])
            x_ref[...] = dx

            @pl.when(layer == 1)
            def _():
                x_ref[...] = x_ref[...].astype(BF).astype(F32)

            for which in range(1, layers):

                @pl.when(layer == which)
                def _(which=which):
                    for copy in saved_copies(which):
                        copy.start()

            return carry

        lax.fori_loop(0, layers, backward, 0)

        chip = me // 2

        def emit(values, piece, at):
            for n in sorted(values)[::2]:
                own = jnp.where(core == 0, values[n], values[n + 1])
                other = jnp.where(core == 0, values[n + 1], values[n])
                offset = chip ^ (n // 2)
                grads[2 * piece][slot_of_chip(offset, core, bits, piece), at] = own.astype(BF)
                grads[2 * piece + 1][slot_of_chip(offset, 1 - core, bits, piece), at] = other.astype(BF)

        copies = []
        for layer in range(1, layers):
            copies += saved_copies(layer)

        def emit_columns(first, cot, act):
            value = mm_tn(cot, act)
            count = value.shape[0] // cin
            base = first // cin
            emit({base + i: value[i * cin : (i + 1) * cin] for i in range(count)}, 0, slice(0, cin))

        for part in range(3):
            emit_columns(part * d, c_dqkv[0, :, part * d : (part + 1) * d], c_u[0])
        emit_columns(3 * d, c_dy[0], c_o[0])
        for part in range(ff // d):
            emit_columns(4 * d + part * d, c_dpre[0, :, part * d : (part + 1) * d], c_u2[0])
        width = members * ROWS16
        column = lax.broadcasted_iota(jnp.int32, (d, width), 1)
        row = lax.broadcasted_iota(jnp.int32, (d, width), 0)
        inner = column % ROWS16
        sel = ((inner < dpc) & (row == (column // ROWS16) * dpc + inner)).astype(BF)
        dob_pad[...] = mm(x_ref[...].astype(BF), sel).astype(BF)
        extra = jnp.concatenate([mm(pcat[...], dob_pad[...]), jnp.zeros((d - patch - tok, width), F32)], 0).T
        dob_pad[...] = mm(c_dout[0], sel).astype(BF)
        parts = ff // d
        share = -(-dpc // parts)
        out_row = lax.broadcasted_iota(jnp.int32, (width, d), 0) % ROWS16
        for part in range(parts):
            value = mm_tn(dob_pad[...], c_h[0, :, part * d : (part + 1) * d])
            moved = pltpu.roll(extra, (dpc - share * part) % width, 0)
            value = jnp.where((out_row >= dpc) & (out_row < dpc + share), moved, value)
            emit(
                {n: value[n * ROWS16 : (n + 1) * ROWS16] for n in range(members)},
                0 if part == 0 else 1,
                slice(cin_pad, cin_pad + ROWS16) if part == 0 else slice((part - 1) * ROWS16, part * ROWS16),
            )
        for copy in copies:
            copy.wait()

    wide = 4 * d + ff
    saved = [d, d, d, ff, 3 * d, d, ff, d]
    out_shape = [
        jax.ShapeDtypeStruct((1, images), F32),
        jax.ShapeDtypeStruct((classes, d), F32),
    ] + [jax.ShapeDtypeStruct((chips, height, d), BF) for height in heights for _ in range(2)]
    out_shape = out_shape + [pltpu.HBM((layers - 1, rows, w), BF) for w in saved]
    any_spec = pl.BlockSpec(memory_space=pl.ANY)
    hbm = pl.BlockSpec(memory_space=pltpu.HBM)
    smem = pl.BlockSpec(memory_space=pltpu.SMEM)
    vmem = pl.BlockSpec(memory_space=pltpu.VMEM)
    n_sems = 3 + (layers - 1) * 2 * group + (layers - 1) * 8 + 3
    scratch = [
        pltpu.VMEM((layers, d, wide), BF),
        pltpu.VMEM((layers, ff, d), BF),
        pltpu.SMEM((capacity,), jnp.int32),
        pltpu.VMEM((rows, d), F32),
        pltpu.VMEM((rows, d), F32),
        pltpu.VMEM((rows, 3 * d), F32),
        pltpu.VMEM((layers, rows, 3 * d), BF),
        pltpu.VMEM((layers, halves * pairs * 2, tok, LANES), F32),
        pltpu.VMEM((layers, rows, ff), BF),
        pltpu.VMEM((layers, rows, 1), F32),
        pltpu.VMEM((layers, rows, 1), F32),
        pltpu.VMEM((halves * pairs, 2 * LANES, LANES), F32),
        pltpu.VMEM((halves * pairs, 2 * LANES, LANES), BF),
        pltpu.VMEM((halves * pairs, 2 * LANES, LANES), BF),
        pltpu.VMEM((patch + tok, d), BF),
        pltpu.VMEM((classes, members // group, d), BF),
    ]
    scratch += [pltpu.VMEM((layers, rows, w), BF) for w in saved]
    scratch += [
        pltpu.VMEM((patch + tok, rows), BF),
        pltpu.VMEM((rows, members * ROWS16), BF),
    ]
    scratch += [
        pltpu.SemaphoreType.DMA((n_sems,)),
    ]
    return pl.pallas_call(
        kernel,
        name="chain",
        in_specs=[smem, smem, vmem] + [hbm] * (5 + 2 * len(pieces)),
        out_specs=[vmem] * (2 + 2 * PIECES) + [hbm] * (len(out_shape) - 2 - 2 * PIECES),
        out_shape=out_shape,
        scratch_shapes=scratch,
        compiler_params=pltpu.CompilerParams(vmem_limit_bytes=cfg['vmem']),
    )


def make_pack(cfg):
    members, group, patch = cfg["members"], cfg["group"], cfg["patch"]
    packed, width = patch // group, LANES // group

    def kernel(patches, out):
        lane = lax.broadcasted_iota(jnp.int32, (packed, LANES), 1)
        parts = [patches[s * packed : (s + 1) * packed].astype(F32) for s in range(group)]
        for j in range(group):
            value = parts[0]
            for s in range(group):
                moved = pltpu.roll(parts[s], (width * (s - j)) % LANES, 1)
                value = jnp.where(lane // width == s, moved, value)
            value = value.astype(BF)
            for shard in range(members // group):
                out[shard * group + j] = value

    return pl.pallas_call(
        kernel,
        name="pack",
        out_shape=jax.ShapeDtypeStruct((members, packed, LANES), BF),
    )


def make_stage(shapes):
    count = len(shapes)

    def kernel(*refs):
        sources, targets, local, sems = refs[:count], refs[count : 2 * count], refs[2 * count : -1], refs[-1]
        loads = [pltpu.make_async_copy(sources[i], local[i], sems.at[i]) for i in range(count)]
        stores = [pltpu.make_async_copy(local[i], targets[i], sems.at[count + i]) for i in range(count)]
        for copy in loads:
            copy.start()
        for load, store in zip(loads, stores):
            load.wait()
            store.start()
        for copy in stores:
            copy.wait()

    return pl.pallas_call(
        kernel,
        name="stage",
        in_specs=[pl.BlockSpec(memory_space=pl.ANY)] * count,
        out_specs=[pl.BlockSpec(memory_space=pltpu.HBM)] * count,
        out_shape=[pltpu.HBM(shape, BF) for shape in shapes],
        scratch_shapes=[pltpu.VMEM(shape, BF) for shape in shapes] + [pltpu.SemaphoreType.DMA((2 * count,))],
        compiler_params=pltpu.CompilerParams(vmem_limit_bytes=16 * 2**20),
    )


def make_server_grads(cfg):
    d, ff, group, layers = cfg["d"], cfg["ff"], cfg["group"], cfg["layers"]
    rows_in, rows_down = d // group, ff // group
    wide = 4 * d + ff
    half = group // 2
    count = layers - 1
    rows = cfg["capacity"] * cfg["pr"]
    saved = [d, d, d, ff, 3 * d, d, ff, d]

    def kernel(*refs):
        sources, refs = refs[:8], refs[8:]
        k_in, s_in, k_down, s_down = refs[:4]
        local, t_in, t_down, sems = refs[4:12], refs[12], refs[13], refs[14]
        rank = lax.axis_index("client") % group

        def loads(layer):
            return [
                pltpu.make_async_copy(src.at[layer], dst.at[layer], sems.at[8 * layer + i])
                for i, (src, dst) in enumerate(zip(sources, local))
            ]

        def stores(layer):
            out = []
            for p in range(group):
                owner = rank ^ p
                o_in, o_down = (k_in, k_down) if p < half else (s_in, s_down)
                at_in = pl.ds(pl.multiple_of(owner * rows_in, rows_in), rows_in)
                at_down = pl.ds(pl.multiple_of(owner * rows_down, rows_down), rows_down)
                sem = 8 * count + 2 * (layer * group + p)
                out.append(pltpu.make_async_copy(t_in.at[layer, at_in], o_in.at[p % half, layer], sems.at[sem]))
                out.append(
                    pltpu.make_async_copy(t_down.at[layer, at_down], o_down.at[p % half, layer], sems.at[sem + 1])
                )
            return out

        for layer in range(count):
            for copy in loads(layer):
                copy.start()

        def compute(layer, carry):
            for which in range(count):

                @pl.when(layer == which)
                def _(which=which):
                    for copy in loads(which):
                        copy.wait()

            u, o, u2, h, dqkv, dy, dpre, dout = [ref.at[layer] for ref in local]
            for part in range(3):
                cs = slice(part * d, (part + 1) * d)
                t_in[layer, :, cs] = mm_tn(u[...], dqkv[:, cs]).astype(BF)
            t_in[layer, :, 3 * d : 4 * d] = mm_tn(o[...], dy[...]).astype(BF)
            for part in range(ff // d):
                cs = slice(part * d, (part + 1) * d)
                t_in[layer, :, 4 * d + part * d : 4 * d + (part + 1) * d] = mm_tn(u2[...], dpre[:, cs]).astype(BF)
                t_down[layer, cs] = mm_tn(h[:, cs], dout[...]).astype(BF)
            for which in range(count):

                @pl.when(layer == which)
                def _(which=which):
                    for copy in stores(which):
                        copy.start()

            return carry

        lax.fori_loop(0, count, compute, 0)
        for layer in range(count):
            for copy in stores(layer):
                copy.wait()

    flops = 2 * rows * (d * wide + ff * d) * count
    any_spec = pl.BlockSpec(memory_space=pl.ANY)
    return pl.pallas_call(
        kernel,
        name="server_grads",
        in_specs=[any_spec] * 8,
        out_specs=[any_spec] * 4,
        out_shape=[jax.ShapeDtypeStruct((half, count, rows_in, wide), BF)] * 2
        + [jax.ShapeDtypeStruct((half, count, rows_down, d), BF)] * 2,
        scratch_shapes=[pltpu.VMEM((count, rows, w), BF) for w in saved]
        + [
            pltpu.VMEM((count, d, wide), BF),
            pltpu.VMEM((count, ff, d), BF),
            pltpu.SemaphoreType.DMA((8 * count + 2 * count * group,)),
        ],
        cost_estimate=pl.CostEstimate(flops=flops * 2, bytes_accessed=16 * 2**20, transcendentals=0),
        compiler_params=pltpu.CompilerParams(vmem_limit_bytes=20 * 1024 * 1024),
    )


def make_finish(cfg):
    d, ff, tok, patch = cfg["d"], cfg["ff"], cfg["tok"], cfg["patch"]
    members, cin, group = cfg["members"], cfg["cin"], cfg["group"]
    classes = cfg["classes"]
    dpc, rows_in = d // members, d // group

    heights, cin_pad = cfg["heights"], cfg["cin_pad"]
    parts = ff // d
    share = -(-dpc // parts)

    def kernel(a0, a1, b, cls, g_embed, g_pos, g_in, g_down, g_class):
        first = a0[0].astype(F32) + b[0, : heights[0]].astype(F32)
        g_in[...] = first[:cin]
        rest = a1[0].astype(F32) + b[0, heights[0] :].astype(F32)
        total = jnp.concatenate([first[cin_pad:], rest], axis=0)
        extra = []
        for part in range(parts):
            block = total[part * ROWS16 : (part + 1) * ROWS16]
            g_down[:, part * d : (part + 1) * d] = block[:dpc]
            if share * part < dpc:
                extra.append(block[dpc : dpc + min(share, dpc - share * part)])
        extra = jnp.concatenate(extra, axis=0)
        g_embed[...] = extra[:, :patch]
        padded = jnp.concatenate([extra[:, patch : patch + tok], jnp.zeros((ROWS16 - dpc, tok), F32)], axis=0)
        g_pos[...] = padded.T[:, :dpc]
        rank = lax.axis_index("client") % group
        value = cls[:, :rows_in]
        for r in range(1, group):
            value = jnp.where(rank == r, cls[:, r * rows_in : (r + 1) * rows_in], value)
        g_class[...] = value

    return pl.pallas_call(
        kernel,
        name="finish",
        out_shape=[
            jax.ShapeDtypeStruct((dpc, patch), F32),
            jax.ShapeDtypeStruct((tok, dpc), F32),
            jax.ShapeDtypeStruct((cin, d), F32),
            jax.ShapeDtypeStruct((dpc, ff), F32),
            jax.ShapeDtypeStruct((classes, rows_in), F32),
        ],
        compiler_params=pltpu.CompilerParams(vmem_limit_bytes=32 * 1024 * 1024),
    )


def swap_bit(block, bit):
    count = lax.axis_size("client")
    return lax.ppermute(block, "client", [(i, i ^ (1 << bit)) for i in range(count)])


def swap_by_core(block, even, odd):
    count = lax.axis_size("client")
    return lax.ppermute(
        block, "client", [(i, i ^ (1 << (even if i % 2 == 0 else odd))) for i in range(count)]
    )


def per_device(
    patches,
    labels,
    assign,
    patch_embed,
    positions,
    client_in,
    client_down,
    server_in,
    server_down,
    classifier,
):
    members = lax.axis_size("client")
    group = members // SHARDS
    group_bits = group.bit_length() - 1
    bits = members.bit_length() - 1
    patch, d = patch_embed.shape
    tok = positions.shape[0]
    ff = client_down.shape[0]
    img = labels.shape[0] // members
    layers = server_in.shape[0] + 1
    pr = patches.shape[0] // group
    cin = client_in.shape[1] // members
    capacity = SLOTS * group

    pieces, first = [1], [0]
    piece_in, piece_down = [server_in[None]], [server_down[None]]
    for bit in range(group_bits):
        whole_in = piece_in[0] if bit == 0 else jnp.concatenate(piece_in, 0)
        whole_down = piece_down[0] if bit == 0 else jnp.concatenate(piece_down, 0)
        piece_in.append(swap_bit(whole_in, bit))
        piece_down.append(swap_bit(whole_down, bit))
        first.append(1 << bit)
        pieces.append(1 << bit)

    cfg = dict(
        d=d,
        ff=ff,
        tok=tok,
        patch=patch,
        members=members,
        group=group,
        capacity=capacity,
        pr=pr,
        images=capacity * pr // tok,
        classes=classifier.shape[2],
        layers=layers,
        bits=bits,
        cin=cin,
        cin_pad=-(-cin // ROWS16) * ROWS16,
        heights=[-(-cin // ROWS16) * ROWS16 + ROWS16, (ff // d - 1) * ROWS16],
        vmem=(47 if bits <= 5 else 58) * 2**20,
        pieces=pieces,
        first=first,
        packed=patch // group,
        img=img,
    )
    others = piece_in[1:] + piece_down[1:]
    others = make_stage([array.shape for array in others])(*others)
    piece_in[1:], piece_down[1:] = others[:group_bits], others[group_bits:]

    outgoing = make_pack(cfg)(patches.T)
    arrived = lax.all_to_all(outgoing, "client", split_axis=0, concat_axis=0, tiled=True)
    results = make_chain(cfg)(
        assign.reshape(-1),
        labels,
        arrived,
        *[
            pltpu.with_memory_space_constraint(array, pltpu.HBM)
            for array in (
                patch_embed,
                positions,
                client_in,
                client_down,
                *piece_in,
                *piece_down,
                classifier.transpose(2, 0, 1),
            )
        ],
    )
    losses, dcls = results[:2]
    grads = results[2 : 2 + 2 * PIECES]
    saved = results[2 + 2 * PIECES :]

    keeps, sends = list(grads[0::2]), list(grads[1::2])
    for bit in range(group_bits):
        dcls = dcls + swap_bit(dcls, bit)
    recvs = [swap_bit(send, 0) for send in sends]
    for step in range(bits - 1):
        for piece in range(PIECES):
            keep, recv = keeps[piece], recvs[piece]
            half = keep.shape[0] // 2
            sends[piece] = (keep[half:].astype(F32) + recv[half:].astype(F32)).astype(BF)
            keeps[piece] = (keep[:half].astype(F32) + recv[:half].astype(F32)).astype(BF)
        if step == 0:
            sends, saved, dcls = lax.optimization_barrier((sends, saved, dcls))
        if step == bits - 2:
            parts = make_server_grads(cfg)(*[pltpu.with_memory_space_constraint(array, pltpu.HBM) for array in saved])
            keep_in, send_in, keep_down, send_down = parts
            for bit in range(group_bits - 1, -1, -1):
                recv_in, recv_down = swap_bit(send_in, bit), swap_bit(send_down, bit)
                if bit == 0:
                    sends, keep_in, keep_down = lax.optimization_barrier((sends, keep_in, keep_down))
                got_in = keep_in.astype(F32) + recv_in.astype(F32)
                got_down = keep_down.astype(F32) + recv_down.astype(F32)
                half = got_in.shape[0] // 2
                keep_in, send_in = got_in[:half], got_in[half:].astype(BF)
                keep_down, send_down = got_down[:half], got_down[half:].astype(BF)
        if step == bits - 2:
            recvs = swap_bit(jnp.concatenate(sends, axis=1), bits - 1)
            continue
        for piece in range(PIECES):
            even, odd = [order[step] for order in stage_orders(bits, piece)]
            recvs[piece] = swap_by_core(sends[piece], even, odd)
    recvs, got_in, got_down = lax.optimization_barrier((recvs, got_in, got_down))
    g_embed, g_pos, g_client_in, g_client_down, g_class = make_finish(cfg)(*keeps, recvs, dcls)

    return (
        losses,
        g_embed.T,
        g_pos,
        g_client_in.T,
        g_client_down.T,
        got_in[0],
        got_down[0],
        g_class.T,
    )


def solution(mesh):
    in_specs = (
        P("client", None),
        P(),
        P(),
        P(),
        P(),
        P(),
        P(),
        P(None, "client", None),
        P(None, "client", None),
        P(),
    )
    out_specs = (
        P("client", None),
        P(None, "client"),
        P(None, "client"),
        P(None, "client"),
        P(None, "client"),
        P(None, "client", None),
        P(None, "client", None),
        P("client", None),
    )
    return jax.shard_map(
        per_device, mesh=mesh, in_specs=in_specs, out_specs=out_specs, check_vma=False
    )
```
